8 devices in a mesh: replica: 2 (over z, y), data: 4 (over x, core).
Axes of the slice: x: 2, y: 2, z: 1, core: 2. Of those that a mesh axis runs over, the one named last changes fastest.
Arguments:
- x_seq: bfloat16 [256, 16, 512], P(('replica', 'data'))
- dy_seq: float32 [256, 16, 512], P(('replica', 'data'))
- w_stack: bfloat16 [2, 1024, 2048], replicated
- b_stack: float32 [2, 2048], replicated
Outputs:
- output 1: float32 [2, 1024, 2048], replicated
- output 2: float32 [2, 2048], replicated
- output 3: float32 [256, 16, 512], P(('replica', 'data'))
All inputs are finite; a program needn't handle non-finite values.
Results may differ from the reference program's by a relative error of at most 0.0120277.
Values are sent between devices in bfloat16 or wider.
A program may use at most 1 GiB of HBM per device.

```python
import jax
import jax.numpy as jnp
from jax import lax

HIDDEN = 512
LAYERS = 2
BATCH_DEV = 32
SEQ = 16
REPLICA = 2
DATA = 4


def setup_inputs(seed: int = 0) -> dict:
    shards = REPLICA * DATA
    batch_rows = BATCH_DEV * shards
    key_list = jax.random.split(jax.random.key(seed), 4)
    x_seq = jax.random.normal(key_list[0], (batch_rows, SEQ, HIDDEN), jnp.float32).astype(jnp.bfloat16)
    dy_seq = jax.random.normal(key_list[1], (batch_rows, SEQ, HIDDEN), jnp.float32)
    w_scale = 1.5 * (2 * HIDDEN) ** -0.5
    w_stack = (jax.random.normal(key_list[2], (LAYERS, 2 * HIDDEN, 4 * HIDDEN), jnp.float32) * w_scale).astype(jnp.bfloat16)
    gate_shift = jnp.concatenate([jnp.ones((2 * HIDDEN,), jnp.float32), jnp.zeros((HIDDEN,), jnp.float32), jnp.ones((HIDDEN,), jnp.float32)])
    b_stack = gate_shift + 0.5 * jax.random.normal(key_list[3], (LAYERS, 4 * HIDDEN), jnp.float32)
    return {'x_seq': x_seq, 'dy_seq': dy_seq, 'w_stack': w_stack, 'b_stack': b_stack}


def layer_forward(u_seq, w_layer, b_layer):
    batch_rows = u_seq.shape[1]

    def time_step(carry_state, u_step):
        h_prev, c_prev = carry_state
        z_all = jnp.dot(jnp.concatenate([u_step, h_prev], axis=-1), w_layer, preferred_element_type=jnp.float32) + b_layer
        z_i, z_f, z_g, z_o = jnp.split(z_all, 4, axis=-1)
        gate_i = jax.nn.sigmoid(z_i)
        gate_f = jax.nn.sigmoid(z_f)
        gate_g = jnp.tanh(z_g)
        gate_o = jax.nn.sigmoid(z_o)
        c_new = gate_f * c_prev + gate_i * gate_g
        tanh_c = jnp.tanh(c_new)
        h_new = (gate_o * tanh_c).astype(jnp.bfloat16)
        return (h_new, c_new), (h_new, c_new, tanh_c, gate_i, gate_f, gate_g, gate_o)

    init_state = (jnp.zeros((batch_rows, HIDDEN), jnp.bfloat16), jnp.zeros((batch_rows, HIDDEN), jnp.float32))
    return lax.scan(time_step, init_state, u_seq)[1]


def layer_backward(u_seq, w_layer, saved_acts, dh_seq):
    h_seq, c_seq, tanh_seq, i_seq, f_seq, g_seq, o_seq = saved_acts
    h_prev_seq = jnp.concatenate([jnp.zeros_like(h_seq[:1]), h_seq[:-1]], axis=0)
    c_prev_seq = jnp.concatenate([jnp.zeros_like(c_seq[:1]), c_seq[:-1]], axis=0)

    def time_step(carry_state, step_in):
        dh_rec, dc_next = carry_state
        dh_out, c_prev, tanh_c, gate_i, gate_f, gate_g, gate_o = step_in
        dh_tot = dh_out + dh_rec
        dc_cur = dc_next + dh_tot * gate_o * (1.0 - tanh_c * tanh_c)
        dz_all = jnp.concatenate([dc_cur * gate_g * gate_i * (1.0 - gate_i), dc_cur * c_prev * gate_f * (1.0 - gate_f), dc_cur * gate_i * (1.0 - gate_g * gate_g), dh_tot * tanh_c * gate_o * (1.0 - gate_o)], axis=-1)
        dz_low = dz_all.astype(jnp.bfloat16)
        du_all = jnp.dot(dz_low, w_layer.T, preferred_element_type=jnp.float32)
        return (du_all[:, HIDDEN:], dc_cur * gate_f), (dz_low, du_all[:, :HIDDEN], jnp.sum(dz_all, axis=0))

    init_state = (jnp.zeros_like(dh_seq[0]), jnp.zeros_like(dh_seq[0]))
    dz_seq, dx_seq, db_steps = lax.scan(time_step, init_state, (dh_seq, c_prev_seq, tanh_seq, i_seq, f_seq, g_seq, o_seq), reverse=True)[1]
    uh_seq = jnp.concatenate([u_seq, h_prev_seq], axis=-1)
    row_count = uh_seq.shape[0] * uh_seq.shape[1]
    dw_layer = jnp.dot(uh_seq.reshape(row_count, 2 * HIDDEN).T, dz_seq.reshape(row_count, 4 * HIDDEN), preferred_element_type=jnp.float32)
    return dw_layer, jnp.sum(db_steps, axis=0), dx_seq


def shard_grads(x_rows, dy_rows, w_stack, b_stack):
    u_first = jnp.swapaxes(x_rows, 0, 1)

    def fwd_layer(u_seq, layer_in):
        saved_acts = layer_forward(u_seq, layer_in[0], layer_in[1])
        return saved_acts[0], (u_seq, saved_acts)

    layer_inputs, layer_saved = lax.scan(fwd_layer, u_first, (w_stack, b_stack))[1]

    def bwd_layer(dh_seq, layer_in):
        dw_layer, db_layer, dx_seq = layer_backward(layer_in[1], layer_in[0], layer_in[2], dh_seq)
        return dx_seq, (dw_layer, db_layer)

    dx_seq, grads = lax.scan(bwd_layer, jnp.swapaxes(dy_rows, 0, 1), (w_stack, layer_inputs, layer_saved), reverse=True)
    return grads[0], grads[1], jnp.swapaxes(dx_seq, 0, 1)


def reference(x_seq, dy_seq, w_stack, b_stack):
    shards = REPLICA * DATA
    x_parts = x_seq.reshape(shards, BATCH_DEV, SEQ, HIDDEN)
    dy_parts = dy_seq.reshape(shards, BATCH_DEV, SEQ, HIDDEN)

    def add_shard(totals, shard_in):
        dw_all, db_all, dx_rows = shard_grads(shard_in[0], shard_in[1], w_stack, b_stack)
        dw_sum = totals[0] + dw_all.astype(jnp.bfloat16).astype(jnp.float32)
        db_sum = totals[1] + db_all.astype(jnp.bfloat16).astype(jnp.float32)
        return (dw_sum, db_sum), dx_rows

    init_totals = (jnp.zeros(w_stack.shape, jnp.float32), jnp.zeros(b_stack.shape, jnp.float32))
    totals, dx_parts = lax.scan(add_shard, init_totals, (x_parts, dy_parts))
    return totals[0], totals[1], dx_parts.reshape(x_seq.shape)
```

```python
import jax
import jax.numpy as jnp
from jax import lax
from jax.experimental import pallas as pl
from jax.experimental.pallas import tpu as pltpu
from jax.sharding import PartitionSpec as P

F32, BF16 = jnp.float32, jnp.bfloat16
MESH = pl.DeviceIdType.MESH
T, B, H = 16, 32, 512
G, R = 4 * H, T * B
C = 32


def dot(a, b):
    return jnp.dot(a, b, preferred_element_type=F32)


def dot_nt(a, b):
    return lax.dot_general(a, b, (((1,), (1,)), ((), ())), preferred_element_type=F32)


def sigmoid(z):
    return 0.5 * jnp.tanh(0.5 * z) + 0.5


def rows(start, n, m=16):
    return pl.ds(start, n) if isinstance(start, int) else pl.ds(pl.multiple_of(start, m), n)


def step_kernel(x_hbm, dy_hbm, w_hbm, b_ref, res, dbo, dxo,
                xv, xf, dyv, w, wt, hb, gt, cb, tc, dz, eb, dbacc, dbs, dbb, dbr, dwb, rp, r1, r2,
                lsem, s_rp, v_rp, s_1, v_1, s_2, v_2, s_a, v_a, s_p, v_p, s_db, v_db):
    rep = lax.axis_index("replica")
    dat = lax.axis_index("data")
    mx, core = dat // 2, dat % 2
    partner = (rep, dat + 1 - 2 * core)
    x_nbr = (rep, lax.rem(dat + 2, 4))
    y_nbr = (1 - rep, dat)
    nbr = ((x_nbr, y_nbr), (y_nbr, x_nbr))
    bits = ((mx, rep), (rep, mx))

    def remote(src, dst, s, v, dev):
        return pltpu.make_async_remote_copy(src_ref=src, dst_ref=dst, send_sem=s, recv_sem=v,
                                            device_id=dev, device_id_type=MESH)

    others = [(lax.rem(rep + (d // 4), 2), lax.rem(dat + (d % 4), 4)) for d in range(1, 8)]
    barrier = pltpu.get_barrier_semaphore()
    for dev in others:
        pl.semaphore_signal(barrier, inc=1, device_id=dev, device_id_type=MESH)

    ld_x = [pltpu.make_async_copy(x_hbm.at[:, pl.ds(k * 128, 128)], xv.at[k], lsem.at[k]) for k in range(4)]
    ld_dy = [pltpu.make_async_copy(dy_hbm.at[:, pl.ds(k * 128, 128)], dyv.at[k], lsem.at[4 + k]) for k in range(4)]
    ld_w = [pltpu.make_async_copy(w_hbm.at[l, pl.ds(k * H, H), pl.ds(j * 256, 256)], w.at[l, k, j],
                                  lsem.at[8 + (2 * l + k) * 8 + j])
            for l in range(2) for k in range(2) for j in range(8)]
    for c in ld_x + ld_w + ld_dy:
        c.start()
    for c in ld_x:
        c.wait()
    xf[...] = xv[...].astype(F32)
    for l in range(2):
        hb[l + 1, pl.ds(0, B), :] = jnp.zeros((B, H), BF16)
        cb[l, pl.ds(0, B), :] = jnp.zeros((B, H), F32)

    @pl.loop(0, T)
    def _(t):
        hb[0, rows((t + 1) * B, B), :] = jnp.concatenate(
            [xf[k, pl.ds(t, B, stride=T), :] for k in range(4)], axis=1).astype(BF16)

    def in_proj(l):
        u = hb[l, pl.ds(B, R), :]
        for j in range(8):
            gt[l, j // 2, :, (j % 2) * 256:(j % 2) * 256 + 256] = dot(u, w[l, 0, j]) + b_ref[l:l + 1, j * 256:(j + 1) * 256]

    def fwd_step(l, t):
        r0, r1_ = rows(t * B, B), rows((t + 1) * B, B)
        h_prev = hb[l + 1, r0, :]
        z = [None] * 4
        for k in (0, 2, 1, 3):
            z[k] = gt[l, k, r0, :] + jnp.concatenate([dot(h_prev, w[l, 1, 2 * k + n]) for n in range(2)], axis=1)
        i, g, f, o = sigmoid(z[0]), jnp.tanh(z[2]), sigmoid(z[1]), sigmoid(z[3])
        c = f * cb[l, r0, :] + i * g
        th = jnp.tanh(c)
        for k, v in enumerate((i, f, g, o)):
            gt[l, k, r0, :] = v
        cb[l, r1_, :] = c
        tc[l, r0, :] = th
        hb[l + 1, r1_, :] = (o * th).astype(BF16)

    def transpose_rec(l):
        @pl.loop(0, 8)
        def _(j):
            for n in range(2):
                wt[l, n, rows(j * 256, 256), :] = w[l, 1, j, pl.ds(n * 256, 256), :].T

    for c in ld_w[:8]:
        c.wait()
    in_proj(0)
    for c in ld_w[8:]:
        c.wait()
    for l in range(2):
        if l:
            in_proj(l)
        pl.loop(0, T)(lambda t, l=l: fwd_step(l, t))
        transpose_rec(l)

    for c in ld_dy:
        c.wait()
    dbacc[...] = jnp.zeros_like(dbacc)

    def bwd_layer(l, e_of):
        def body(s, carry):
            r, dc_next = carry
            t = T - 1 - s
            r0 = rows(t * B, B)
            i, f, g, o = [gt[l, k, r0, :] for k in range(4)]
            th, c_prev = tc[l, r0, :], cb[l, r0, :]
            dh = e_of(t) + r
            dc = dc_next + dh * o * (1.0 - th * th)
            dzs = (dc * g * i * (1.0 - i), dc * c_prev * f * (1.0 - f), dc * i * (1.0 - g * g), dh * th * o * (1.0 - o))
            acc = None
            for k, d in enumerate(dzs):
                dbacc[l, :, k * H:(k + 1) * H] += d[0:8] + d[8:16] + d[16:24] + d[24:32]
                d16 = d.astype(BF16)
                for n in range(2):
                    dz[l, 2 * k + n, r0, :] = d16[:, n * 256:(n + 1) * 256]
                p = [dot(d16, wt[l, n, pl.ds(k * H, H), :]) for n in range(2)]
                acc = p if acc is None else [a + b for a, b in zip(acc, p)]
            return jnp.concatenate(acc, axis=1), dc * f

        zero = jnp.zeros((B, H), F32)
        lax.fori_loop(0, T, body, (zero, zero))

    def dx_of(l, put):
        acc = None
        for m in range(2):
            rr = pl.ds(m * 256, 256)
            acc = None
            for j in range(8):
                p = dot_nt(dz[l, j, rr, :], w[l, 0, j])
                acc = p if acc is None else acc + p
            put(m, acc)

    def block_row(who, q, grp):
        b1 = bits[q][0]
        part = 1 - b1 if grp == 0 else b1
        return who * H + q * 256 + part * 128

    def dw_block(l, who, q, grp):
        r0 = block_row(who, q, grp)
        lhs = hb[l + who, rows(B * (1 - who), R, B), rows(r0 - who * H, 128, 128)]
        lt = lhs.T
        for n in range(8):
            dwb[l, rows(r0, 128), n * 256:(n + 1) * 256] = dot(lt, dz[l, n]).astype(BF16)

    def cp_rp(l, q, grp):
        rr = rows(block_row(1 - core, q, grp), 128)
        return remote(dwb.at[l, rr], rp.at[l, q, grp], s_rp.at[l, q, grp], v_rp.at[l, q, grp], partner)

    def add_rows(l, r0, src, n):
        @pl.loop(0, n // 16)
        def _(i):
            rr = rows(r0 + i * 16, 16)
            dwb[l, rr, :] = (dwb[l, rr, :].astype(F32) + src[rows(i * 16, 16), :].astype(F32)).astype(BF16)

    def piece(q, i, kept):
        b1, b2 = bits[q]
        half = 1 - b2 if i < 2 else b2
        return block_row(core, q, 1 if kept else 0) + 64 * half + C * (i % 2)

    def cp_1(l, q, i):
        return remote(dwb.at[l, rows(piece(q, i, False), C)], r1.at[l, q, i], s_1.at[l, q, i], v_1.at[l, q, i], nbr[q][0])

    def cp_2(l, q, i):
        return remote(dwb.at[l, rows(piece(q, i, True), C)], r2.at[l, q, i], s_2.at[l, q, i], v_2.at[l, q, i], nbr[q][1])

    def fin_row(q, k, i):
        b1, b2 = bits[q]
        c1 = b1 if k in (0, 1) else 1 - b1
        c2 = b2 if k in (0, 2) else 1 - b2
        return core * H + q * 256 + c1 * 128 + c2 * 64 + C * i

    def cp_a(l, q, k, i):
        rr = rows(fin_row(q, 1 if k == 2 else 0, i), C)
        return remote(res.at[l, rr], res.at[l, rr], s_a.at[l, q, k, i], v_a.at[l, q, k, i], nbr[q][1 if k == 0 else 0])

    def cp_p(l, q, k, i):
        rr = rows(fin_row(q, k, i), C)
        return remote(res.at[l, rr], res.at[l, rr], s_p.at[l, q, k, i], v_p.at[l, q, k, i], partner)

    QI = [(q, i) for i in range(2) for q in range(2)]

    def grads_send(l):
        for q in range(2):
            dw_block(l, 1 - core, q, 0)
            cp_rp(l, q, 0).start()
        for q in range(2):
            dw_block(l, core, q, 0)
        for q in range(2):
            cp_rp(l, q, 0).wait_recv()
            add_rows(l, block_row(core, q, 0), rp.at[l, q, 0], 128)
            for i in range(4):
                cp_1(l, q, i).start()
        for q in range(2):
            dw_block(l, 1 - core, q, 1)
            cp_rp(l, q, 1).start()
        for q in range(2):
            dw_block(l, core, q, 1)
        for q in range(2):
            cp_rp(l, q, 1).wait_recv()
            add_rows(l, block_row(core, q, 1), rp.at[l, q, 1], 128)

    def recv_1(l, half):
        for q, i in QI:
            i += 2 * half
            cp_1(l, q, i).wait_recv()
            add_rows(l, piece(q, i, True), r1.at[l, q, i], C)
            if half == 0:
                cp_2(l, q, i).start()

    def recv_2(l):
        for q, i in QI:
            cp_2(l, q, i).wait_recv()
            src, dst = piece(q, i + 2, True), fin_row(q, 0, i)

            @pl.loop(0, C // 16)
            def _(m):
                res[l, rows(dst + m * 16, 16), :] = (
                    dwb[l, rows(src + m * 16, 16), :].astype(F32) + r2[l, q, i, rows(m * 16, 16), :].astype(F32)).astype(BF16)
            cp_a(l, q, 0, i).start()
            cp_a(l, q, 1, i).start()
            cp_p(l, q, 0, i).start()

    def recv_a1(l):
        for q, i in QI:
            cp_a(l, q, 0, i).wait_recv()
            cp_a(l, q, 2, i).start()
            cp_p(l, q, 1, i).start()

    def recv_a2(l, k):
        for q, i in QI:
            cp_a(l, q, k, i).wait_recv()
            cp_p(l, q, k + 1, i).start()

    bwd_layer(1, lambda t: jnp.concatenate([dyv[k, pl.ds(t, B, stride=T), :] for k in range(4)], axis=1))
    pl.semaphore_wait(barrier, 7)
    grads_send(1)

    def put_e(m, v):
        eb[pl.ds(m * 256, 256), :] = v
    dx_of(1, put_e)
    bwd_layer(0, lambda t: eb[rows(t * B, B), :])
    recv_1(1, 0)
    grads_send(0)

    for l in range(2):
        for j in range(8):
            dbs[8 * l + j:8 * l + j + 1, :] = jnp.sum(dbacc[l, :, j * 256:(j + 1) * 256], axis=0, keepdims=True)
    dbb[...] = dbs[...].astype(BF16)
    me = rep * 4 + dat
    cps = [remote(dbb, dbr.at[d - 1], s_db.at[d - 1], v_db.at[d - 1], dev) for d, dev in enumerate(others, 1)]
    for c in cps:
        c.start()

    def put_dx(m, v):
        for s in range(8):
            for k in range(4):
                dxo[k, pl.ds(8 * m + s, B, stride=T), :] = v[s * B:(s + 1) * B, k * 128:(k + 1) * 128]
    dx_of(0, put_dx)

    recv_1(1, 1)
    recv_2(1)
    recv_a1(1)
    recv_1(0, 0)
    recv_1(0, 1)
    recv_a2(1, 1)
    recv_a2(1, 2)
    recv_2(0)
    recv_a1(0)
    for c in cps:
        c.wait_recv()
    tot = dbb[...].astype(F32)
    for d in range(7):
        tot += dbr[d].astype(F32)
    dbo[...] = tot
    recv_a2(0, 1)
    recv_a2(0, 2)
    for l in (1, 0):
        for q in range(2):
            for grp in range(2):
                cp_rp(l, q, grp).wait_send()
            for i in range(4):
                cp_1(l, q, i).wait_send()
            for i in range(2):
                cp_2(l, q, i).wait_send()
                for k in range(3):
                    cp_a(l, q, k, i).wait_send()
                for k in range(4):
                    cp_p(l, q, k, i).wait_send()
                    cp_p(l, q, k, i).wait_recv()
    for c in cps:
        c.wait_send()


def out_kernel(res, dbo, dxo, dw_ref, db_ref, dx_ref, buf, sem, xsem):
    cx = [pltpu.make_async_copy(dxo.at[k], dx_ref.at[:, pl.ds(k * 128, 128)], xsem.at[k]) for k in range(4)]
    for c in cx:
        c.start()
    n = 128

    def cp(s, slot):
        return pltpu.make_async_copy(buf.at[slot], dw_ref.at[s // 8, rows(lax.rem(s, 8) * n, n)], sem.at[slot])

    @pl.loop(0, 16)
    def _(s):
        slot = lax.rem(s, 4)

        @pl.when(s >= 4)
        def _():
            cp(s - 4, slot).wait()

        @pl.loop(0, n // 16)
        def _(i):
            buf[slot, rows(i * 16, 16), :] = res[s // 8, rows(lax.rem(s, 8) * n + i * 16, 16), :].astype(F32)
        cp(s, slot).start()
    for l in range(2):
        for j in range(8):
            db_ref[l:l + 1, j * 256:(j + 1) * 256] = dbo[8 * l + j:8 * l + j + 1, :]
    for s in range(12, 16):
        cp(s, s % 4).wait()
    for c in cx:
        c.wait()


def solution(mesh):
    vm = pl.BlockSpec(memory_space=pltpu.VMEM)
    hbm = pl.BlockSpec(memory_space=pl.ANY)
    dma = pltpu.SemaphoreType.DMA

    def local_step(x, dy, w, b):
        scratch = [
            pltpu.VMEM((4, R, 128), BF16), pltpu.VMEM((4, R, 128), F32), pltpu.VMEM((4, R, 128), F32),
            pltpu.VMEM((2, 2, 8, H, 256), BF16), pltpu.VMEM((2, 2, G, 256), BF16), pltpu.VMEM((3, R + B, H), BF16),
            pltpu.VMEM((2, 4, R, H), F32), pltpu.VMEM((2, R + B, H), F32), pltpu.VMEM((2, R, H), F32),
            pltpu.VMEM((2, 8, R, 256), BF16), pltpu.VMEM((R, H), F32), pltpu.VMEM((2, 8, G), F32),
            pltpu.VMEM((16, 256), F32), pltpu.VMEM((16, 256), BF16), pltpu.VMEM((7, 16, 256), BF16),
            pltpu.VMEM((2, 2 * H, G), BF16), pltpu.VMEM((2, 2, 2, 128, G), BF16),
            pltpu.VMEM((2, 2, 4, C, G), BF16), pltpu.VMEM((2, 2, 2, C, G), BF16),
            dma((40,)), dma((2, 2, 2)), dma((2, 2, 2)), dma((2, 2, 4)), dma((2, 2, 4)), dma((2, 2, 2)), dma((2, 2, 2)),
            dma((2, 2, 3, 2)), dma((2, 2, 3, 2)), dma((2, 2, 4, 2)), dma((2, 2, 4, 2)), dma((7,)), dma((7,)),
        ]
        res, dbo, dxo = pl.pallas_call(
            step_kernel,
            out_shape=(jax.ShapeDtypeStruct((2, 2 * H, G), BF16), jax.ShapeDtypeStruct((16, 256), F32),
                       jax.ShapeDtypeStruct((4, R, 128), F32)),
            in_specs=[hbm, hbm, hbm, vm], out_specs=(vm, vm, vm), scratch_shapes=scratch,
            compiler_params=pltpu.CompilerParams(collective_id=0, has_side_effects=True, vmem_limit_bytes=63 * 1024 * 1024),
        )(x.reshape(R, H), dy.reshape(R, H), w, b)
        dw, db, dx = pl.pallas_call(
            out_kernel,
            out_shape=(jax.ShapeDtypeStruct((2, 2 * H, G), F32), jax.ShapeDtypeStruct((2, G), F32),
                       jax.ShapeDtypeStruct((R, H), F32)),
            in_specs=[vm, vm, vm], out_specs=(hbm, vm, hbm),
            scratch_shapes=[pltpu.VMEM((4, 128, G), F32), dma((4,)), dma((4,))],
            compiler_params=pltpu.CompilerParams(vmem_limit_bytes=32 * 1024 * 1024),
        )(res, dbo, dxo)
        return dw, db, dx.reshape(B, T, H)

    rows_spec = P(("replica", "data"))
    return jax.shard_map(local_step, mesh=mesh, in_specs=(rows_spec, rows_spec, P(), P()),
                         out_specs=(P(), P(), rows_spec), check_vma=False)
```

```python
import jax
import jax.numpy as jnp
from jax import lax
from jax.experimental import pallas as pl
from jax.experimental.pallas import tpu as pltpu
from jax.sharding import PartitionSpec as P

F32, BF16 = jnp.float32, jnp.bfloat16
MESH = pl.DeviceIdType.MESH
T, B, H = 16, 32, 512
G, R = 4 * H, T * B
ORDER = (0, 1, 2, 3)
PAD = 24
VMEM_LIMIT = 54 * 1024 * 1024
C = 64


def dot(a, b):
    return jnp.dot(a, b, preferred_element_type=F32)


def dot_nt(a, b):
    return lax.dot_general(a, b, (((1,), (1,)), ((), ())), preferred_element_type=F32)


def sigmoid(z):
    return 0.5 * jnp.tanh(0.5 * z) + 0.5


def rows(start, n, m=16):
    return pl.ds(start, n) if isinstance(start, int) else pl.ds(pl.multiple_of(start, m), n)


def step_kernel(x_hbm, dy_hbm, w_hbm, b_hbm, res, dbo, dxo,
                b_ref, xv, xf, dyv, w, wt, hb, gt, cb, tc, dz, eb, dbacc, dbs, dbb, dbr, dwb, rp, r1, r2,
                lsem, s_rp, v_rp, s_1, v_1, s_2, v_2, s_a, v_a, s_p, v_p, s_db, v_db):
    rep = lax.axis_index("replica")
    dat = lax.axis_index("data")
    mx, core = dat // 2, dat % 2
    partner = (rep, dat + 1 - 2 * core)
    x_nbr = (rep, lax.rem(dat + 2, 4))
    y_nbr = (1 - rep, dat)
    nbr = ((x_nbr, y_nbr), (y_nbr, x_nbr))
    bits = ((mx, rep), (rep, mx))

    def remote(src, dst, s, v, dev):
        return pltpu.make_async_remote_copy(src_ref=src, dst_ref=dst, send_sem=s, recv_sem=v,
                                            device_id=dev, device_id_type=MESH)

    others = [(lax.rem(rep + (d // 4), 2), lax.rem(dat + (d % 4), 4)) for d in range(1, 8)]
    barrier = pltpu.get_barrier_semaphore()

    ld_x = [pltpu.make_async_copy(x_hbm.at[:, pl.ds(k * 128, 128)], xv.at[k], lsem.at[0]) for k in range(4)]
    ld_dy = [pltpu.make_async_copy(dy_hbm.at[:, pl.ds(k * 128, 128)], dyv.at[k], lsem.at[1]) for k in range(4)]
    ld_w = [pltpu.make_async_copy(w_hbm.at[l, pl.ds(k * H, H), pl.ds(j * 256, 256)], w.at[l, k, j],
                                  lsem.at[2 + 2 * l + k])
            for l in range(2) for k in range(2) for j in range(8)]
    ld_b = pltpu.make_async_copy(b_hbm, b_ref, lsem.at[6])
    for c in ld_x + [ld_b] + ld_w[:16]:
        c.start()
    for dev in others:
        pl.semaphore_signal(barrier, inc=1, device_id=dev, device_id_type=MESH)
    for l in range(2):
        hb[l + 1, pl.ds(0, B), :] = jnp.zeros((B, H), BF16)
        cb[l, pl.ds(0, B), :] = jnp.zeros((B, H), F32)
    pltpu.make_async_copy(xv, xv, lsem.at[0]).wait()
    for i in range(B):
        xf[:, i * PAD:i * PAD + T, :] = xv[:, i * T:(i + 1) * T, :].astype(F32)

    @pl.loop(0, T)
    def _(t):
        hb[0, rows((t + 1) * B, B), :] = jnp.concatenate(
            [xf[k, pl.ds(t, B, stride=PAD), :] for k in range(4)], axis=1).astype(BF16)
    for c in ld_w[16:] + ld_dy:
        c.start()

    def wait_w(l, k):
        pltpu.make_async_copy(w.at[l, k], w.at[l, k], lsem.at[2 + 2 * l + k]).wait()

    ld_b.wait()
    wait_w(0, 0)

    def in_block(l, s, n, m=128):
        r0 = rows(s * 128, m)
        gt[l, n // 2, r0, (n % 2) * 256:(n % 2) * 256 + 256] = (
            dot(hb[l, rows(B + s * 128, m), :], w[l, 0, n]) + b_ref[l:l + 1, n * 256:(n + 1) * 256])

    def transpose_rec(l, j, n):
        wt[l, n, rows(j * 256, 256), :] = w[l, 1, j, pl.ds(n * 256, 256), :].T

    def step_dots(l, t, h):
        zin = [gt[l, k, rows(t * B, B), :] for k in range(4)]
        prod = [None] * 8
        for k in (0, 2, 1, 3):
            for n in range(2):
                prod[2 * k + n] = dot(h, w[l, 1, 2 * k + n])
        return zin, prod

    def step_gates(l, t, zp, c):
        zin, prod = zp
        r0, r1_ = rows(t * B, B), rows((t + 1) * B, B)
        hs, cs = [], []
        for n in range(2):
            m = slice(n * 256, (n + 1) * 256)
            z = [zin[k][:, m] + prod[2 * k + n] for k in range(4)]
            i, g, f, o = sigmoid(z[0]), jnp.tanh(z[2]), sigmoid(z[1]), sigmoid(z[3])
            cn = f * c[:, m] + i * g
            th = jnp.tanh(cn)
            hn = (o * th).astype(BF16)
            for k, v in enumerate((i, f, g, o)):
                gt[l, k, r0, m] = v
            cb[l, r1_, m] = cn
            tc[l, r0, m] = th
            hb[l + 1, r1_, m] = hn
            hs.append(hn)
            cs.append(cn)
        return jnp.concatenate(hs, axis=1), jnp.concatenate(cs, axis=1)

    zero_state = (jnp.zeros((B, H), BF16), jnp.zeros((B, H), F32))
    for n in range(8):
        in_block(0, 0, n)
    for n in range(8):
        in_block(0, 2, n, 256)
    wait_w(0, 1)
    h0, c0 = zero_state
    for q in range(4):
        zp = step_dots(0, q, h0)
        in_block(0, 1, 2 * q)
        in_block(0, 1, 2 * q + 1)
        transpose_rec(0, q // 2, q % 2)
        h0, c0 = step_gates(0, q, zp, c0)
    wait_w(1, 0)
    wait_w(1, 1)

    def both(s, carry):
        h0, c0, h1, c1 = carry
        t0, t1 = 4 * s + 4, 4 * s
        a = step_dots(0, t0, h0)
        for n in range(8):
            in_block(1, s, n)
        h0, c0 = step_gates(0, t0, a, c0)
        for q in range(4):
            if q < 3:
                a = step_dots(0, t0 + q + 1, h0)
            b = step_dots(1, t1 + q, h1)
            if q < 3:
                h0, c0 = step_gates(0, t0 + q + 1, a, c0)
            transpose_rec(0, 2 * s + 2 + q // 2, q % 2)
            transpose_rec(1, 2 * s + q // 2, q % 2)
            h1, c1 = step_gates(1, t1 + q, b, c1)
        return h0, c0, h1, c1

    h0, c0, h1, c1 = lax.fori_loop(0, 3, both, (h0, c0) + zero_state)
    for n in range(8):
        in_block(1, 3, n)
    for q in range(4):
        zp = step_dots(1, 12 + q, h1)
        transpose_rec(1, 6 + q // 2, q % 2)
        h1, c1 = step_gates(1, 12 + q, zp, c1)

    pltpu.make_async_copy(dyv, dyv, lsem.at[1]).wait()
    dbacc[...] = jnp.zeros_like(dbacc)

    def bwd_layer(l, e_of, halfway=None):
        def body(s, carry):
            r, dc_next = carry
            t = T - 1 - s
            r0 = rows(t * B, B)
            i, f, g, o = [gt[l, k, r0, :] for k in range(4)]
            th, c_prev = tc[l, r0, :], cb[l, r0, :]
            dh = e_of(t) + r
            dc = dc_next + dh * o * (1.0 - th * th)
            dzs = (dc * g * i * (1.0 - i), dc * c_prev * f * (1.0 - f), dc * i * (1.0 - g * g), dh * th * o * (1.0 - o))
            acc = None
            for k in ORDER:
                d = dzs[k]
                dbacc[l, :, k * H:(k + 1) * H] += d[0:8] + d[8:16] + d[16:24] + d[24:32]
                d16 = d.astype(BF16)
                for n in range(2):
                    dz[l, 2 * k + n, r0, :] = d16[:, n * 256:(n + 1) * 256]
                p = [dot(d16, wt[l, n, pl.ds(k * H, H), :]) for n in range(2)]
                acc = p if acc is None else [a + b for a, b in zip(acc, p)]
            return jnp.concatenate(acc, axis=1), dc * f

        zero = jnp.zeros((B, H), F32)
        carry = (zero, zero)
        if halfway is None:
            lax.fori_loop(0, T, body, carry)
        else:
            carry = lax.fori_loop(0, T // 2, body, carry)
            halfway()
            lax.fori_loop(T // 2, T, body, carry)

    def dx_of(l, put):
        acc = None
        for m in range(2):
            rr = pl.ds(m * 256, 256)
            acc = None
            for j in range(8):
                p = dot_nt(dz[l, j, rr, :], w[l, 0, j])
                acc = p if acc is None else acc + p
            put(m, acc)

    def block_row(who, q, grp):
        b1 = bits[q][0]
        part = 1 - b1 if grp == 0 else b1
        return who * H + q * 256 + part * 128

    def cols(half):
        return pl.ds(pl.multiple_of(half * 1024, 1024), 1024)

    def half_of(q, h):
        b2 = bits[q][1]
        return 1 - b2 if h == 0 else b2

    def lhs_of(l, who, q, grp):
        r0 = block_row(who, q, grp)
        return hb[l + who, rows(B * (1 - who), R, B), rows(r0 - who * H, 128, 128)].T

    def dw_block(l, who, q, grp, h):
        lt = lhs_of(l, who, q, grp)
        half = half_of(q, h)
        for n in range(4):
            dwb[l, rows(block_row(who, q, grp), 128), pl.ds(pl.multiple_of(half * 1024 + n * 256, 256), 256)] = (
                dot(lt, dz[l, 4 * half + n]).astype(BF16))

    def cp_rp(l, q, grp, h):
        rr, cc = rows(block_row(1 - core, q, grp), 128), cols(half_of(q, h))
        return remote(dwb.at[l, rr, cc], rp.at[l, q, grp, h], s_rp, v_rp.at[l, q, grp, h], partner)

    def add_rp(l, q, grp, h):
        r0, cc = block_row(core, q, grp), cols(half_of(q, h))

        @pl.loop(0, 4)
        def _(i):
            rr = rows(r0 + i * 32, 32)
            dwb[l, rr, cc] = (dwb[l, rr, cc].astype(F32) + rp[l, q, grp, h, rows(i * 32, 32), :].astype(F32)).astype(BF16)

    def place(q, grp, h, i):
        return rows(block_row(core, q, grp) + C * i, C), cols(half_of(q, h))

    def cp_1(l, q, h, i):
        rr, cc = place(q, 0, h, i)
        return remote(dwb.at[l, rr, cc], r1.at[l, q, h, i], s_1, v_1.at[l, q, h, i], nbr[q][0])

    def cp_2(l, q, i):
        rr, cc = place(q, 1, 0, i)
        return remote(dwb.at[l, rr, cc], r2.at[l, q, i], s_2, v_2.at[l, q, i], nbr[q][1])

    def fin(q, k, i):
        b1, b2 = bits[q]
        c1 = b1 if k in (0, 1) else 1 - b1
        c2 = b2 if k in (0, 2) else 1 - b2
        return rows(core * H + q * 256 + c1 * 128 + C * i, C), cols(c2)

    def cp_a(l, q, k, i):
        rr, cc = fin(q, 1 if k == 2 else 0, i)
        return remote(res.at[l, rr, cc], res.at[l, rr, cc], s_a, v_a.at[l, q, k, i], nbr[q][1 if k == 0 else 0])

    def cp_p(l, q, k, i):
        rr, cc = fin(q, k, i)
        return remote(res.at[l, rr, cc], res.at[l, rr, cc], s_p, v_p, partner)

    QI = [(q, i) for i in range(2) for q in range(2)]

    def dw_pair(l, who, grp, h):
        for q in range(2):
            dw_block(l, who, q, grp, h)
            if who is not core:
                cp_rp(l, q, grp, h).start()

    def take_rp(l, grp, h):
        for q in range(2):
            cp_rp(l, q, grp, h).wait_recv()
            add_rp(l, q, grp, h)
            if grp == 0:
                for i in range(2):
                    cp_1(l, q, h, i).start()

    def grads_send(l):
        other = 1 - core
        dw_pair(l, other, 0, 0)
        dw_pair(l, core, 0, 0)
        dw_pair(l, other, 0, 1)
        take_rp(l, 0, 0)
        dw_pair(l, core, 0, 1)
        dw_pair(l, other, 1, 0)
        take_rp(l, 0, 1)
        dw_pair(l, core, 1, 0)
        dw_pair(l, other, 1, 1)
        dw_pair(l, core, 1, 1)

    def recv_1(l, h):
        if h == 0:
            take_rp(l, 1, 0)
            take_rp(l, 1, 1)
        for q, i in QI:
            cp_1(l, q, h, i).wait_recv()
            rr, cc = place(q, 1, h, i)
            dwb[l, rr, cc] = (dwb[l, rr, cc].astype(F32) + r1[l, q, h, i].astype(F32)).astype(BF16)
            if h == 0:
                cp_2(l, q, i).start()

    def recv_2(l):
        for q, i in QI:
            cp_2(l, q, i).wait_recv()
            rr, cc = fin(q, 0, i)
            res[l, rr, cc] = (dwb[l, rr, cc].astype(F32) + r2[l, q, i].astype(F32)).astype(BF16)
            cp_a(l, q, 0, i).start()
            cp_p(l, q, 0, i).start()

    def send_a1(l):
        for q, i in QI:
            cp_a(l, q, 1, i).start()

    def recv_a1(l):
        for q, i in QI:
            cp_a(l, q, 0, i).wait_recv()
            cp_a(l, q, 2, i).start()
            cp_p(l, q, 1, i).start()

    def recv_a2(l, k):
        for q, i in QI:
            cp_a(l, q, k, i).wait_recv()
            cp_p(l, q, k + 1, i).start()

    bwd_layer(1, lambda t: jnp.concatenate([dyv[k, pl.ds(t, B, stride=T), :] for k in range(4)], axis=1))
    pl.semaphore_wait(barrier, 7)
    grads_send(1)

    def put_e(m, v):
        eb[pl.ds(m * 256, 256), :] = v
    dx_of(1, put_e)
    bwd_layer(0, lambda t: eb[rows(t * B, B), :], lambda: recv_1(1, 0))
    grads_send(0)

    for l in range(2):
        for j in range(8):
            dbs[8 * l + j:8 * l + j + 1, :] = jnp.sum(dbacc[l, :, j * 256:(j + 1) * 256], axis=0, keepdims=True)
    dbb[...] = dbs[...].astype(BF16)
    me = rep * 4 + dat
    cps = [remote(dbb, dbr.at[d - 1], s_db, v_db, dev) for d, dev in enumerate(others, 1)]
    for c in cps:
        c.start()

    def put_dx(m, v):
        for s in range(8):
            for k in range(4):
                dxo[k, pl.ds(8 * m + s, B, stride=T), :] = v[s * B:(s + 1) * B, k * 128:(k + 1) * 128]

    recv_1(1, 1)
    recv_2(1)
    dx_of(0, put_dx)
    recv_1(0, 0)
    send_a1(1)
    recv_1(0, 1)
    recv_a1(1)
    recv_2(0)
    send_a1(0)
    recv_a2(1, 1)
    recv_a2(1, 2)
    remote(dbr, dbr, s_db, v_db, partner).wait_recv()
    tot = dbb[...].astype(F32)
    for d in range(7):
        tot += dbr[d].astype(F32)
    dbo[...] = tot
    recv_a1(0)
    recv_a2(0, 1)
    recv_a2(0, 2)
    half_w = dwb.at[:, pl.ds(0, H)]
    remote(half_w, half_w, s_rp, v_p, partner).wait_send()
    quarter = dwb.at[:, pl.ds(0, 256)]
    remote(quarter, quarter, s_1, v_p, partner).wait_send()
    eighth = dwb.at[:, pl.ds(0, 128)]
    remote(eighth, eighth, s_2, v_p, partner).wait_send()
    part = dwb.at[:, pl.ds(0, 384)]
    remote(part, part, s_a, v_p, partner).wait_send()
    mine = res.at[:, rows(core * H, H)]
    theirs = res.at[:, rows((1 - core) * H, H)]
    remote(mine, theirs, s_p, v_p, partner).wait()
    remote(dbr, dbr, s_db, v_db, partner).wait_send()


def out_kernel(res, dbo, dxo, dw_ref, db_ref, dx_ref, buf, dbv, sem, xsem):
    cx = [pltpu.make_async_copy(dxo.at[k], dx_ref.at[:, pl.ds(k * 128, 128)], xsem.at[k]) for k in range(4)]
    for l in range(2):
        for j in range(8):
            dbv[l:l + 1, j * 256:(j + 1) * 256] = dbo[8 * l + j:8 * l + j + 1, :]
    cx.append(pltpu.make_async_copy(dbv, db_ref, xsem.at[4]))
    for c in cx:
        c.start()
    n = 64

    def cp(s):
        return pltpu.make_async_copy(buf.at[s], dw_ref.at[s // 16, rows(lax.rem(s, 16) * n, n)], sem)

    @pl.loop(0, 32)
    def _(s):
        buf[s] = res[s // 16, rows(lax.rem(s, 16) * n, n), :].astype(F32)
        cp(s).start()

    pltpu.make_async_copy(buf, buf, sem).wait()
    for c in cx:
        c.wait()


def solution(mesh):
    vm = pl.BlockSpec(memory_space=pltpu.VMEM)
    hbm = pl.BlockSpec(memory_space=pl.ANY)
    dma = pltpu.SemaphoreType.DMA

    def local_step(x, dy, w, b):
        scratch = [
            pltpu.VMEM((2, G), F32),
            pltpu.VMEM((4, R, 128), BF16), pltpu.VMEM((4, B * PAD, 128), F32), pltpu.VMEM((4, R, 128), F32),
            pltpu.VMEM((2, 2, 8, H, 256), BF16), pltpu.VMEM((2, 2, G, 256), BF16), pltpu.VMEM((3, R + B, H), BF16),
            pltpu.VMEM((2, 4, R, H), F32), pltpu.VMEM((2, R + B, H), F32), pltpu.VMEM((2, R, H), F32),
            pltpu.VMEM((2, 8, R, 256), BF16), pltpu.VMEM((R, H), F32), pltpu.VMEM((2, 8, G), F32),
            pltpu.VMEM((16, 256), F32), pltpu.VMEM((16, 256), BF16), pltpu.VMEM((7, 16, 256), BF16),
            pltpu.VMEM((2, 2 * H, G), BF16), pltpu.VMEM((2, 2, 2, 2, 128, 1024), BF16),
            pltpu.VMEM((2, 2, 2, 2, C, 1024), BF16), pltpu.VMEM((2, 2, 2, C, 1024), BF16),
            dma((7,)), dma, dma((2, 2, 2, 2)), dma, dma((2, 2, 2, 2)), dma, dma((2, 2, 2)),
            dma, dma((2, 2, 3, 2)), dma, dma, dma, dma,
        ]
        res, dbo, dxo = pl.pallas_call(
            step_kernel,
            out_shape=(pltpu.VMEM((2, 2 * H, G), BF16), pltpu.VMEM((16, 256), F32), pltpu.VMEM((4, R, 128), F32)),
            in_specs=[hbm, hbm, hbm, hbm], out_specs=(vm, vm, vm), scratch_shapes=scratch,
            compiler_params=pltpu.CompilerParams(collective_id=0, has_side_effects=True, vmem_limit_bytes=VMEM_LIMIT),
        )(x.reshape(R, H), dy.reshape(R, H), w, b)
        dw, db, dx = pl.pallas_call(
            out_kernel,
            out_shape=(jax.ShapeDtypeStruct((2, 2 * H, G), F32), jax.ShapeDtypeStruct((2, G), F32),
                       jax.ShapeDtypeStruct((R, H), F32)),
            in_specs=[vm, vm, vm], out_specs=(hbm, hbm, hbm),
            scratch_shapes=[pltpu.VMEM((32, 64, G), F32), pltpu.VMEM((2, G), F32), dma, dma((5,))],
            compiler_params=pltpu.CompilerParams(vmem_limit_bytes=32 * 1024 * 1024),
        )(res, dbo, dxo)
        return dw, db, dx.reshape(B, T, H)

    rows_spec = P(("replica", "data"))
    return jax.shard_map(local_step, mesh=mesh, in_specs=(rows_spec, rows_spec, P(), P()),
                         out_specs=(P(), P(), rows_spec), check_vma=False)
```

```python
import jax
import jax.numpy as jnp
from jax import lax
from jax.experimental import pallas as pl
from jax.experimental.pallas import tpu as pltpu
from jax.sharding import PartitionSpec as P

F32, BF16 = jnp.float32, jnp.bfloat16
MESH = pl.DeviceIdType.MESH
T, B, H = 16, 32, 512
G, R = 4 * H, T * B
ORDER = (0, 1, 2, 3)
PAD = 24
CUT = (5, 13)
VMEM_LIMIT = 54 * 1024 * 1024
C = 64


def dot(a, b):
    return jnp.dot(a, b, preferred_element_type=F32)


def dot_nt(a, b):
    return lax.dot_general(a, b, (((1,), (1,)), ((), ())), preferred_element_type=F32)


def sigmoid(z):
    return 0.5 * jnp.tanh(0.5 * z) + 0.5


def rows(start, n, m=16):
    return pl.ds(start, n) if isinstance(start, int) else pl.ds(pl.multiple_of(start, m), n)


def step_kernel(x_hbm, dy_hbm, w_hbm, b_hbm, res, dbo, dxo,
                b_ref, xv, xf, dyv, w, wt, hb, gt, cb, tc, dz, eb, dbacc, dbs, dbb, dbr, dwb, rp, r1, r2,
                hx, zx, ub, rph, r1h, r2u, r2h,
                lsem, s_rp, v_rp, s_1, v_1, s_2, v_2, s_a, v_a, s_p, v_p, s_db, v_db,
                s_h, v_h, s_z, v_z, s_rph, v_rph, s_1h, v_1h, s_2x, v_2x, s_ax, v_ax, s_px, v_px):
    rep = lax.axis_index("replica")
    dat = lax.axis_index("data")
    mx, core = dat // 2, dat % 2
    partner = (rep, dat + 1 - 2 * core)
    x_nbr = (rep, lax.rem(dat + 2, 4))
    y_nbr = (1 - rep, dat)
    nbr = ((x_nbr, y_nbr), (y_nbr, x_nbr))
    bits = ((mx, rep), (rep, mx))

    def remote(src, dst, s, v, dev):
        return pltpu.make_async_remote_copy(src_ref=src, dst_ref=dst, send_sem=s, recv_sem=v,
                                            device_id=dev, device_id_type=MESH)

    others = [(lax.rem(rep + (d // 4), 2), lax.rem(dat + (d % 4), 4)) for d in range(1, 8)]
    barrier = pltpu.get_barrier_semaphore()

    ld_x = [pltpu.make_async_copy(x_hbm.at[:, pl.ds(k * 128, 128)], xv.at[k], lsem.at[0]) for k in range(4)]
    ld_dy = [pltpu.make_async_copy(dy_hbm.at[:, pl.ds(k * 128, 128)], dyv.at[k], lsem.at[1]) for k in range(4)]
    ld_w = [pltpu.make_async_copy(w_hbm.at[l, pl.ds(k * H, H), pl.ds(j * 256, 256)], w.at[l, k, j],
                                  lsem.at[2 + 2 * l + k])
            for l in range(2) for k in range(2) for j in range(8)]
    ld_b = pltpu.make_async_copy(b_hbm, b_ref, lsem.at[6])
    for c in ld_x + [ld_b] + ld_w[:16]:
        c.start()
    for dev in others:
        pl.semaphore_signal(barrier, inc=1, device_id=dev, device_id_type=MESH)
    for l in range(2):
        hb[l + 1, pl.ds(0, B), :] = jnp.zeros((B, H), BF16)
        cb[l, pl.ds(0, B), :] = jnp.zeros((B, H), F32)
    pltpu.make_async_copy(xv, xv, lsem.at[0]).wait()
    for i in range(B):
        xf[:, i * PAD:i * PAD + T, :] = xv[:, i * T:(i + 1) * T, :].astype(F32)

    @pl.loop(0, T)
    def _(t):
        hb[0, rows((t + 1) * B, B), :] = jnp.concatenate(
            [xf[k, pl.ds(t, B, stride=PAD), :] for k in range(4)], axis=1).astype(BF16)
    for c in ld_w[16:] + ld_dy:
        c.start()

    def wait_w(l, k):
        pltpu.make_async_copy(w.at[l, k], w.at[l, k], lsem.at[2 + 2 * l + k]).wait()

    ld_b.wait()
    wait_w(0, 0)

    def in_block(l, s, n, m=128):
        r0 = rows(s * 128, m)
        gt[l, n // 2, r0, (n % 2) * 256:(n % 2) * 256 + 256] = (
            dot(hb[l, rows(B + s * 128, m), :], w[l, 0, n]) + b_ref[l:l + 1, n * 256:(n + 1) * 256])

    def transpose_rec(l, j, n):
        wt[l, n, rows(j * 256, 256), :] = w[l, 1, j, pl.ds(n * 256, 256), :].T

    def step_dots(l, t, h):
        zin = [gt[l, k, rows(t * B, B), :] for k in range(4)]
        prod = [None] * 8
        for k in (0, 2, 1, 3):
            for n in range(2):
                prod[2 * k + n] = dot(h, w[l, 1, 2 * k + n])
        return zin, prod

    def step_gates(l, t, zp, c):
        zin, prod = zp
        r0, r1_ = rows(t * B, B), rows((t + 1) * B, B)
        hs, cs = [], []
        for n in range(2):
            m = slice(n * 256, (n + 1) * 256)
            z = [zin[k][:, m] + prod[2 * k + n] for k in range(4)]
            i, g, f, o = sigmoid(z[0]), jnp.tanh(z[2]), sigmoid(z[1]), sigmoid(z[3])
            cn = f * c[:, m] + i * g
            th = jnp.tanh(cn)
            hn = (o * th).astype(BF16)
            for k, v in enumerate((i, f, g, o)):
                gt[l, k, r0, m] = v
            cb[l, r1_, m] = cn
            tc[l, r0, m] = th
            hb[l + 1, r1_, m] = hn
            hs.append(hn)
            cs.append(cn)
        return jnp.concatenate(hs, axis=1), jnp.concatenate(cs, axis=1)

    zero_state = (jnp.zeros((B, H), BF16), jnp.zeros((B, H), F32))
    for n in range(8):
        in_block(0, 0, n)
    for n in range(8):
        in_block(0, 2, n, 256)
    wait_w(0, 1)
    h0, c0 = zero_state
    for q in range(4):
        zp = step_dots(0, q, h0)
        in_block(0, 1, 2 * q)
        in_block(0, 1, 2 * q + 1)
        transpose_rec(0, q // 2, q % 2)
        h0, c0 = step_gates(0, q, zp, c0)
    wait_w(1, 0)
    wait_w(1, 1)

    def pick(a, b):
        return a + core * (b - a)

    u_b1, u_b2 = pick(mx, rep), pick(rep, mx)
    u_n1 = (pick(rep, 1 - rep), pick(lax.rem(dat + 2, 4), dat))
    u_n2 = (pick(1 - rep, rep), pick(dat, lax.rem(dat + 2, 4)))
    x_core0, y_core1 = (rep, 2 * (1 - mx)), (1 - rep, 2 * mx + 1)
    dests = ((partner, 0, pick(4 + 2 * rep, 2 * mx)), (x_core0, 1 + core, 2 * (1 - mx)), (y_core1, 1 + core, 4 + 2 * (1 - rep)))
    u_col = pick(2 * mx, 4 + 2 * rep)

    def send_h(s):
        for dev, slot, _ in dests:
            remote(hb.at[1, rows(B + s * 128, 128)], hx.at[slot, rows(s * 128, 128)], s_h, v_h.at[slot], dev).start()

    def send_z(r0, n):
        for dev, slot, c0 in dests:
            remote(dz.at[1, pl.ds(c0, 2), rows(r0, n)], zx.at[slot, :, rows(r0, n)], s_z, v_z.at[slot], dev).start()

    pl.semaphore_wait(barrier, 7)

    def both(s, carry):
        h0, c0, h1, c1 = carry
        t0, t1 = 4 * s + 4, 4 * s
        send_h(s)
        a = step_dots(0, t0, h0)
        for n in range(8):
            in_block(1, s, n)
        h0, c0 = step_gates(0, t0, a, c0)
        for q in range(4):
            if q < 3:
                a = step_dots(0, t0 + q + 1, h0)
            b = step_dots(1, t1 + q, h1)
            if q < 3:
                h0, c0 = step_gates(0, t0 + q + 1, a, c0)
            transpose_rec(0, 2 * s + 2 + q // 2, q % 2)
            transpose_rec(1, 2 * s + q // 2, q % 2)
            h1, c1 = step_gates(1, t1 + q, b, c1)
        return h0, c0, h1, c1

    h0, c0, h1, c1 = lax.fori_loop(0, 3, both, (h0, c0) + zero_state)
    send_h(3)
    for n in range(8):
        in_block(1, 3, n)
    for q in range(4):
        zp = step_dots(1, 12 + q, h1)
        transpose_rec(1, 6 + q // 2, q % 2)
        h1, c1 = step_gates(1, 12 + q, zp, c1)

    pltpu.make_async_copy(dyv, dyv, lsem.at[1]).wait()
    dbacc[...] = jnp.zeros_like(dbacc)

    def bwd_layer(l, e_of, halfway=None, every_2=None):
        def body(s, carry):
            r, dc_next = carry
            t = T - 1 - s
            r0 = rows(t * B, B)
            i, f, g, o = [gt[l, k, r0, :] for k in range(4)]
            th, c_prev = tc[l, r0, :], cb[l, r0, :]
            dh = e_of(t) + r
            dc = dc_next + dh * o * (1.0 - th * th)
            dzs = (dc * g * i * (1.0 - i), dc * c_prev * f * (1.0 - f), dc * i * (1.0 - g * g), dh * th * o * (1.0 - o))
            acc = None
            for k in ORDER:
                d = dzs[k]
                dbacc[l, :, k * H:(k + 1) * H] += d[0:8] + d[8:16] + d[16:24] + d[24:32]
                d16 = d.astype(BF16)
                for n in range(2):
                    dz[l, 2 * k + n, r0, :] = d16[:, n * 256:(n + 1) * 256]
                p = [dot(d16, wt[l, n, pl.ds(k * H, H), :]) for n in range(2)]
                acc = p if acc is None else [a + b for a, b in zip(acc, p)]
            return jnp.concatenate(acc, axis=1), dc * f

        zero = jnp.zeros((B, H), F32)
        carry = (zero, zero)
        if every_2 is not None:
            def two(u, carry):
                carry = body(2 * u, carry)
                carry = body(2 * u + 1, carry)
                every_2((T - 2 - 2 * u) * B)
                return carry
            lax.fori_loop(0, T // 2, two, carry)
        else:
            carry = lax.fori_loop(0, CUT[0], body, carry)
            halfway(0)
            carry = lax.fori_loop(CUT[0], CUT[1], body, carry)
            halfway(1)
            lax.fori_loop(CUT[1], T, body, carry)

    def dx_of(l, put):
        acc = None
        for m in range(2):
            rr = pl.ds(m * 256, 256)
            acc = None
            for j in range(8):
                p = dot_nt(dz[l, j, rr, :], w[l, 0, j])
                acc = p if acc is None else acc + p
            put(m, acc)

    def block_row(who, q, grp):
        b1 = bits[q][0]
        part = 1 - b1 if grp == 0 else b1
        return who * H + q * 256 + part * 128

    def cols(half):
        return pl.ds(pl.multiple_of(half * 1024, 1024), 1024)

    def half_of(q, h):
        b2 = bits[q][1]
        return 1 - b2 if h == 0 else b2

    def lhs_of(l, who, q, grp):
        r0 = block_row(who, q, grp)
        return hb[l + who, rows(B * (1 - who), R, B), rows(r0 - who * H, 128, 128)].T

    def dw_block(l, who, q, grp, h):
        lt = lhs_of(l, who, q, grp)
        half = half_of(q, h)
        for n in range(4):
            dwb[l, rows(block_row(who, q, grp), 128), pl.ds(pl.multiple_of(half * 1024 + n * 256, 256), 256)] = (
                dot(lt, dz[l, 4 * half + n]).astype(BF16))

    def cp_rp(l, q, grp, h):
        rr, cc = rows(block_row(1 - core, q, grp), 128), cols(half_of(q, h))
        return remote(dwb.at[l, rr, cc], rp.at[q, grp, h], s_rp, v_rp.at[q, grp, h], partner)

    def add_rp(l, q, grp, h):
        r0, cc = block_row(core, q, grp), cols(half_of(q, h))

        @pl.loop(0, 4)
        def _(i):
            rr = rows(r0 + i * 32, 32)
            dwb[l, rr, cc] = (dwb[l, rr, cc].astype(F32) + rp[q, grp, h, rows(i * 32, 32), :].astype(F32)).astype(BF16)

    def place(q, grp, h, i):
        return rows(block_row(core, q, grp) + C * i, C), cols(half_of(q, h))

    def cp_1(l, q, h, i):
        rr, cc = place(q, 0, h, i)
        return remote(dwb.at[l, rr, cc], r1.at[q, h, i], s_1, v_1.at[q, h, i], nbr[q][0])

    def cp_2(l, q, i):
        rr, cc = place(q, 1, 0, i)
        return remote(dwb.at[l, rr, cc], r2.at[q, i], s_2, v_2.at[q, i], nbr[q][1])

    def fin(q, k, i):
        b1, b2 = bits[q]
        c1 = b1 if k in (0, 1) else 1 - b1
        c2 = b2 if k in (0, 2) else 1 - b2
        return rows(core * H + q * 256 + c1 * 128 + C * i, C), cols(c2)

    def cp_a(l, q, k, i):
        rr, cc = fin(q, 1 if k == 2 else 0, i)
        return remote(res.at[l, rr, cc], res.at[l, rr, cc], s_a, v_a.at[q, k, i], nbr[q][1 if k == 0 else 0])

    def cp_p(l, q, k, i):
        rr, cc = fin(q, k, i)
        return remote(res.at[l, rr, cc], res.at[l, rr, cc], s_p, v_p, partner)

    QI = [(q, i) for i in range(2) for q in range(2)]

    def dw_pair(l, who, grp, h):
        for q in range(2):
            dw_block(l, who, q, grp, h)
            if who is not core:
                cp_rp(l, q, grp, h).start()

    def take_rp(l, grp, h):
        for q in range(2):
            cp_rp(l, q, grp, h).wait_recv()
            add_rp(l, q, grp, h)
            if grp == 0:
                for i in range(2):
                    cp_1(l, q, h, i).start()

    def grads_send(l):
        other = 1 - core
        dw_pair(l, other, 0, 0)
        dw_pair(l, core, 0, 0)
        dw_pair(l, other, 0, 1)
        take_rp(l, 0, 0)
        dw_pair(l, core, 0, 1)
        dw_pair(l, other, 1, 0)
        take_rp(l, 0, 1)
        dw_pair(l, core, 1, 0)
        dw_pair(l, other, 1, 1)
        dw_pair(l, core, 1, 1)

    def recv_1(l, h):
        if h == 0:
            take_rp(l, 1, 0)
            take_rp(l, 1, 1)
        for q, i in QI:
            cp_1(l, q, h, i).wait_recv()
            rr, cc = place(q, 1, h, i)
            dwb[l, rr, cc] = (dwb[l, rr, cc].astype(F32) + r1[q, h, i].astype(F32)).astype(BF16)
            if h == 0:
                cp_2(l, q, i).start()

    def recv_2(l):
        for q, i in QI:
            cp_2(l, q, i).wait_recv()
            rr, cc = fin(q, 0, i)
            res[l, rr, cc] = (dwb[l, rr, cc].astype(F32) + r2[q, i].astype(F32)).astype(BF16)
            cp_a(l, q, 0, i).start()
            cp_p(l, q, 0, i).start()

    def send_a1(l):
        for q, i in QI:
            cp_a(l, q, 1, i).start()

    def recv_a1(l):
        for q, i in QI:
            cp_a(l, q, 0, i).wait_recv()
            cp_a(l, q, 2, i).start()
            cp_p(l, q, 1, i).start()

    def recv_a2(l, k):
        for q, i in QI:
            cp_a(l, q, k, i).wait_recv()
            cp_p(l, q, k + 1, i).start()

    def h_row(who, q):
        return H + who * 256 + q * 128

    def dwh_block(who, q, grp):
        lt = hb[2, pl.ds(0, R), rows(h_row(who, q) - H, 128, 128)].T
        half = 1 - bits[q][0] if grp == 0 else bits[q][0]
        for n in range(4):
            dwb[1, rows(h_row(who, q), 128), pl.ds(pl.multiple_of(half * 1024 + n * 256, 256), 256)] = (
                dot(lt, dz[1, 4 * half + n]).astype(BF16))

    def cp_rph(q, grp):
        half = 1 - bits[q][0] if grp == 0 else bits[q][0]
        return remote(dwb.at[1, rows(h_row(1 - core, q), 128), cols(half)], rph.at[q, grp], s_rph, v_rph.at[q, grp], partner)

    def quarter(q, grp, h):
        half = 1 - bits[q][0] if grp == 0 else bits[q][0]
        return pl.ds(pl.multiple_of(half * 1024 + 512 * half_of(q, h), 512), 512)

    def cp_1h(q, h):
        return remote(dwb.at[1, rows(h_row(core, q), 128), quarter(q, 0, h)], r1h.at[q, h], s_1h, v_1h.at[q, h], nbr[q][0])

    def take_rph(grp):
        for q in range(2):
            cp_rph(q, grp).wait_recv()
            r0, cc = h_row(core, q), cols(1 - bits[q][0] if grp == 0 else bits[q][0])

            @pl.loop(0, 4)
            def _(i):
                rr = rows(r0 + i * 32, 32)
                dwb[1, rr, cc] = (dwb[1, rr, cc].astype(F32) + rph[q, grp, rows(i * 32, 32), :].astype(F32)).astype(BF16)
            if grp == 0:
                for h in range(2):
                    cp_1h(q, h).start()

    def grads_send_1():
        for grp in range(2):
            for q in range(2):
                dwh_block(1 - core, q, grp)
                cp_rph(q, grp).start()
            for q in range(2):
                dwh_block(core, q, grp)
            if grp == 0:
                take_rph(0)

    def sum_u():
        for i in range(3):
            remote(hx.at[i], hx.at[i], s_h, v_h.at[i], partner).wait_recv()
            remote(zx.at[i], zx.at[i], s_z, v_z.at[i], partner).wait_recv()
        for m in range(4):
            f0 = pl.ds(m * 128, 128)
            lts = [hb[1, pl.ds(B, R), f0].T] + [hx[i, :, f0].T for i in range(3)]
            for n in range(2):
                zs = [dz[1, u_col + n]] + [zx[i, n] for i in range(3)]
                acc = None
                for lt, z in zip(lts, zs):
                    p = dot(lt, z).astype(BF16).astype(F32)
                    acc = p if acc is None else acc + p
                ub[f0, n * 256:(n + 1) * 256] = acc.astype(BF16)

    def item_nbr(j):
        return (u_n1, u_n2) if j < 2 else nbr[j - 2]

    def item_fin(j, k):
        b1, b2 = (u_b1, u_b2) if j < 2 else bits[j - 2]
        c1 = b1 if k in (0, 1) else 1 - b1
        c2 = b2 if k in (0, 2) else 1 - b2
        if j < 2:
            return rows(256 * c2 + 128 * j, 128), pl.ds(pl.multiple_of(core * 1024 + 512 * c1, 512), 512)
        return rows(h_row(core, j - 2), 128), pl.ds(pl.multiple_of(1024 * c1 + 512 * c2, 512), 512)

    def cp_2x(j):
        if j < 2:
            src, dst = ub.at[rows(256 * (1 - u_b2) + 128 * j, 128)], r2u.at[j]
        else:
            src, dst = dwb.at[1, rows(h_row(core, j - 2), 128), quarter(j - 2, 1, 0)], r2h.at[j - 2]
        return remote(src, dst, s_2x, v_2x.at[j], item_nbr(j)[1])

    def cp_ax(j, k):
        rr, cc = item_fin(j, 1 if k == 2 else 0)
        return remote(res.at[1, rr, cc], res.at[1, rr, cc], s_ax, v_ax.at[j, k], item_nbr(j)[1 if k == 0 else 0])

    def cp_px(j, k):
        rr, cc = item_fin(j, k)
        return remote(res.at[1, rr, cc], res.at[1, rr, cc], s_px, v_px, partner)

    JS = (2, 3, 0, 1)

    def recv_1h(h):
        if h == 0:
            take_rph(1)
        for q in range(2):
            cp_1h(q, h).wait_recv()
            rr, cc = rows(h_row(core, q), 128), quarter(q, 1, h)
            dwb[1, rr, cc] = (dwb[1, rr, cc].astype(F32) + r1h[q, h].astype(F32)).astype(BF16)
            if h == 0:
                cp_2x(2 + q).start()

    def recv_2x():
        for j in JS:
            cp_2x(j).wait_recv()
            rr, cc = item_fin(j, 0)
            if j < 2:
                mine, got = ub[rows(256 * u_b2 + 128 * j, 128), :], r2u[j]
            else:
                mine, got = dwb[1, rr, cc], r2h[j - 2]
            res[1, rr, cc] = (mine.astype(F32) + got.astype(F32)).astype(BF16)
            cp_ax(j, 0).start()
            cp_px(j, 0).start()

    def send_a1x():
        for j in JS:
            cp_ax(j, 1).start()

    def recv_a1x():
        for j in JS:
            cp_ax(j, 0).wait_recv()
            cp_ax(j, 2).start()
            cp_px(j, 1).start()

    def recv_a2x(k):
        for j in JS:
            cp_ax(j, k).wait_recv()
            cp_px(j, k + 1).start()

    def between(part):
        if part == 0:
            sum_u()
            for j in range(2):
                cp_2x(j).start()
        else:
            recv_1h(0)

    bwd_layer(1, lambda t: jnp.concatenate([dyv[k, pl.ds(t, B, stride=T), :] for k in range(4)], axis=1), every_2=lambda r0: send_z(r0, 2 * B))
    grads_send_1()

    def put_e(m, v):
        eb[pl.ds(m * 256, 256), :] = v
    dx_of(1, put_e)
    bwd_layer(0, lambda t: eb[rows(t * B, B), :], between)
    grads_send(0)

    for l in range(2):
        for j in range(8):
            dbs[8 * l + j:8 * l + j + 1, :] = jnp.sum(dbacc[l, :, j * 256:(j + 1) * 256], axis=0, keepdims=True)
    dbb[...] = dbs[...].astype(BF16)
    me = rep * 4 + dat
    cps = [remote(dbb, dbr.at[d - 1], s_db, v_db, dev) for d, dev in enumerate(others, 1)]
    for c in cps:
        c.start()

    def put_dx(m, v):
        for s in range(8):
            for k in range(4):
                dxo[k, pl.ds(8 * m + s, B, stride=T), :] = v[s * B:(s + 1) * B, k * 128:(k + 1) * 128]

    recv_1h(1)
    recv_2x()
    dx_of(0, put_dx)
    recv_1(0, 0)
    send_a1x()
    recv_1(0, 1)
    recv_a1x()
    recv_2(0)
    send_a1(0)
    recv_a2x(1)
    recv_a2x(2)
    remote(dbr, dbr, s_db, v_db, partner).wait_recv()
    tot = dbb[...].astype(F32)
    for d in range(7):
        tot += dbr[d].astype(F32)
    dbo[...] = tot
    recv_a1(0)
    recv_a2(0, 1)
    recv_a2(0, 2)
    for n, sem in ((512, s_rp), (256, s_1), (128, s_2), (384, s_a), (256, s_rph), (128, s_1h), (128, s_2x), (384, s_ax)):
        part = dwb.at[0, pl.ds(0, n)]
        remote(part, part, sem, v_p, partner).wait_send()
    remote(hx, hx, s_h, v_p, partner).wait_send()
    remote(zx, zx, s_z, v_p, partner).wait_send()
    for l, snd, rcv in ((0, s_p, v_p), (1, s_px, v_px)):
        half_w = res.at[l, pl.ds(0, H)]
        remote(half_w, half_w, snd, rcv, partner).wait()
    remote(dbr, dbr, s_db, v_db, partner).wait_send()


def out_kernel(res, dbo, dxo, dw_ref, db_ref, dx_ref, buf, dbv, sem, xsem):
    cx = [pltpu.make_async_copy(dxo.at[k], dx_ref.at[:, pl.ds(k * 128, 128)], xsem.at[k]) for k in range(4)]
    for l in range(2):
        for j in range(8):
            dbv[l:l + 1, j * 256:(j + 1) * 256] = dbo[8 * l + j:8 * l + j + 1, :]
    cx.append(pltpu.make_async_copy(dbv, db_ref, xsem.at[4]))
    for c in cx:
        c.start()
    n = 64

    def cp(s):
        return pltpu.make_async_copy(buf.at[s], dw_ref.at[s // 16, rows(lax.rem(s, 16) * n, n)], sem)

    @pl.loop(0, 32)
    def _(s):
        buf[s] = res[s // 16, rows(lax.rem(s, 16) * n, n), :].astype(F32)
        cp(s).start()

    pltpu.make_async_copy(buf, buf, sem).wait()
    for c in cx:
        c.wait()


def solution(mesh):
    vm = pl.BlockSpec(memory_space=pltpu.VMEM)
    hbm = pl.BlockSpec(memory_space=pl.ANY)
    dma = pltpu.SemaphoreType.DMA

    def local_step(x, dy, w, b):
        scratch = [
            pltpu.VMEM((2, G), F32),
            pltpu.VMEM((4, R, 128), BF16), pltpu.VMEM((4, B * PAD, 128), F32), pltpu.VMEM((4, R, 128), F32),
            pltpu.VMEM((2, 2, 8, H, 256), BF16), pltpu.VMEM((2, 2, G, 256), BF16), pltpu.VMEM((3, R + B, H), BF16),
            pltpu.VMEM((2, 4, R, H), F32), pltpu.VMEM((2, R + B, H), F32), pltpu.VMEM((2, R, H), F32),
            pltpu.VMEM((2, 8, R, 256), BF16), pltpu.VMEM((R, H), F32), pltpu.VMEM((2, 8, G), F32),
            pltpu.VMEM((16, 256), F32), pltpu.VMEM((16, 256), BF16), pltpu.VMEM((7, 16, 256), BF16),
            pltpu.VMEM((2, 2 * H, G), BF16), pltpu.VMEM((2, 2, 2, 128, 1024), BF16),
            pltpu.VMEM((2, 2, 2, C, 1024), BF16), pltpu.VMEM((2, 2, C, 1024), BF16),
            pltpu.VMEM((3, R, H), BF16), pltpu.VMEM((3, 2, R, 256), BF16), pltpu.VMEM((H, 512), BF16),
            pltpu.VMEM((2, 2, 128, 1024), BF16), pltpu.VMEM((2, 2, 128, 512), BF16), pltpu.VMEM((2, 128, 512), BF16),
            pltpu.VMEM((2, 128, 512), BF16),
            dma((7,)), dma, dma((2, 2, 2)), dma, dma((2, 2, 2)), dma, dma((2, 2)),
            dma, dma((2, 3, 2)), dma, dma, dma, dma,
            dma, dma((3,)), dma, dma((3,)), dma, dma((2, 2)), dma, dma((2, 2)), dma, dma((4,)), dma, dma((4, 3)), dma, dma,
        ]
        res, dbo, dxo = pl.pallas_call(
            step_kernel,
            out_shape=(pltpu.VMEM((2, 2 * H, G), BF16), pltpu.VMEM((16, 256), F32), pltpu.VMEM((4, R, 128), F32)),
            in_specs=[hbm, hbm, hbm, hbm], out_specs=(vm, vm, vm), scratch_shapes=scratch,
            compiler_params=pltpu.CompilerParams(collective_id=0, has_side_effects=True, vmem_limit_bytes=VMEM_LIMIT),
        )(x.reshape(R, H), dy.reshape(R, H), w, b)
        dw, db, dx = pl.pallas_call(
            out_kernel,
            out_shape=(jax.ShapeDtypeStruct((2, 2 * H, G), F32), jax.ShapeDtypeStruct((2, G), F32),
                       jax.ShapeDtypeStruct((R, H), F32)),
            in_specs=[vm, vm, vm], out_specs=(hbm, hbm, hbm),
            scratch_shapes=[pltpu.VMEM((32, 64, G), F32), pltpu.VMEM((2, G), F32), dma, dma((5,))],
            compiler_params=pltpu.CompilerParams(vmem_limit_bytes=32 * 1024 * 1024),
        )(res, dbo, dxo)
        return dw, db, dx.reshape(B, T, H)

    rows_spec = P(("replica", "data"))
    return jax.shard_map(local_step, mesh=mesh, in_specs=(rows_spec, rows_spec, P(), P()),
                         out_specs=(P(), P(), rows_spec), check_vma=False)
```

```python
import jax
import jax.numpy as jnp
from jax import lax
from jax.experimental import pallas as pl
from jax.experimental.pallas import tpu as pltpu
from jax.sharding import PartitionSpec as P

F32, BF16 = jnp.float32, jnp.bfloat16
MESH = pl.DeviceIdType.MESH
T, B, H = 16, 32, 512
G, R = 4 * H, T * B
ORDER = (0, 1, 2, 3)
PAD = 24
MID = 2
CUT = (6, 13)
TWO, THREE, FOUR, EIGHT = range(2), range(3), range(4), range(8)
W = 256
BLK, QTR, HALF, SUB = 128, 512, 1024, 16
P2, P3 = (2, 2), (2, 2, 2)
VMEM_LIMIT = 54 * 1024 * 1024
C = 64


def flip(bit):
    return 1 - bit


def loop(n):
    return pl.loop(0, n)


def dot(a, b):
    return jnp.dot(a, b, preferred_element_type=F32)


def dot_nt(a, b):
    return lax.dot_general(a, b, (((1,), (1,)), ((), ())), preferred_element_type=F32)


def sigmoid(z):
    return 0.5 * jnp.tanh(0.5 * z) + 0.5


def rows(start, n, m=SUB):
    return pl.ds(start, n) if isinstance(start, int) else pl.ds(pl.multiple_of(start, m), n)


def step_kernel(x_hbm, dy_hbm, w_hbm, b_hbm, res, dbo, dxo,
                b_ref, xv, xf, dyv, w, wt, hb, gt, cb, tc, dz, eb, dbacc, dbs, dbb, dbr, dwb, rp, r1, r2,
                hx, zx, ub, rph, r1h, r2u, r2h,
                lsem, s_rp, v_rp, s_1, v_1, s_2, v_2, s_a, v_a, s_p, v_p, s_db, v_db,
                s_h, v_h, s_z, v_z, s_rph, v_rph, s_1h, v_1h, s_2x, v_2x, s_ax, v_ax, s_px, v_px):
    rep = lax.axis_index("replica")
    dat = lax.axis_index("data")
    mx, core = dat // 2, dat % 2
    partner = (rep, dat + 1 - 2 * core)
    x_nbr = (rep, lax.rem(dat + 2, 4))
    y_nbr = (flip(rep), dat)
    nbr = ((x_nbr, y_nbr), (y_nbr, x_nbr))
    bits = ((mx, rep), (rep, mx))

    def remote(src, dst, s, v, dev):
        return pltpu.make_async_remote_copy(src_ref=src, dst_ref=dst, send_sem=s, recv_sem=v,
                                            device_id=dev, device_id_type=MESH)

    others = [(lax.rem(rep + (d // 4), 2), lax.rem(dat + (d % 4), 4)) for d in range(1, 8)]
    barrier = pltpu.get_barrier_semaphore()

    ld_x = [pltpu.make_async_copy(x_hbm.at[:, pl.ds(k * BLK, BLK)], xv.at[k], lsem.at[0]) for k in FOUR]
    ld_dy = [pltpu.make_async_copy(dy_hbm.at[:, pl.ds(k * BLK, BLK)], dyv.at[k], lsem.at[1]) for k in FOUR]
    ld_w = [pltpu.make_async_copy(w_hbm.at[l, pl.ds(k * H, H), pl.ds(j * W, W)], w.at[l, k, j],
                                  lsem.at[2 + 2 * l + k])
            for l in TWO for k in TWO for j in EIGHT]
    ld_b = pltpu.make_async_copy(b_hbm, b_ref, lsem.at[6])
    for c in ld_x + [ld_b] + ld_w[:8]:
        c.start()
    for dev in others:
        pl.semaphore_signal(barrier, inc=1, device_id=dev, device_id_type=MESH)
    for l in TWO:
        hb[l + 1, pl.ds(0, B), :] = jnp.zeros((B, H), BF16)
        cb[l, pl.ds(0, B), :] = jnp.zeros((B, H), F32)
    pltpu.make_async_copy(xv, xv, lsem.at[0]).wait()
    for c in ld_w[8:SUB]:
        c.start()
    for i in range(B):
        xf[:, i * PAD:i * PAD + T, :] = xv[:, i * T:(i + 1) * T, :].astype(F32)

    @loop(T)
    def _(t):
        hb[0, rows((t + 1) * B, B), :] = jnp.concatenate(
            [xf[k, pl.ds(t, B, stride=PAD), :] for k in FOUR], axis=1).astype(BF16)
    for c in ld_w[SUB:] + ld_dy:
        c.start()

    def wait_w(l, k):
        pltpu.make_async_copy(w.at[l, k], w.at[l, k], lsem.at[2 + 2 * l + k]).wait()

    ld_b.wait()
    pltpu.make_async_copy(w.at[0, 0], w.at[0, 0], lsem.at[2]).wait()

    def in_block(l, s, n, m=BLK):
        r0 = rows(s * BLK, m)
        gt[l, n // 2, r0, W * (n % 2):W * (n % 2) + W] = (
            dot(hb[l, rows(B + s * BLK, m), :], w[l, 0, n]) + b_ref[l:l + 1, W * n:W * n + W])

    def transpose_rec(l, j, n):
        wt[l, n, rows(j * W, W), :] = w[l, 1, j, pl.ds(n * W, W), :].T

    def step_dots(l, t, h):
        zin = [gt[l, k, rows(t * B, B), :] for k in FOUR]
        prod = [None] * 8
        if h is None:
            return zin, prod
        for k in (0, 2, 1, 3):
            for n in TWO:
                prod[2 * k + n] = dot(h, w[l, 1, 2 * k + n])
        return zin, prod

    def step_gates(l, t, zp, c):
        zin, prod = zp
        r0, r1_ = rows(t * B, B), rows((t + 1) * B, B)
        hs, cs = [], []
        for n in TWO:
            m = slice(W * n, W * n + W)
            z = [zin[k][:, m] if prod[2 * k + n] is None else zin[k][:, m] + prod[2 * k + n] for k in FOUR]
            i, g, f, o = sigmoid(z[0]), jnp.tanh(z[2]), sigmoid(z[1]), sigmoid(z[3])
            cn = f * c[:, m] + i * g
            th = jnp.tanh(cn)
            hn = (o * th).astype(BF16)
            for k, v in enumerate((i, f, g, o)):
                gt[l, k, r0, m] = v
            cb[l, r1_, m] = cn
            tc[l, r0, m] = th
            hb[l + 1, r1_, m] = hn
            hs.append(hn)
            cs.append(cn)
        return jnp.concatenate(hs, axis=1), jnp.concatenate(cs, axis=1)

    zero_state = (jnp.zeros((B, H), BF16), jnp.zeros((B, H), F32))
    for n in EIGHT:
        in_block(0, 0, n)
    h0, c0 = None, zero_state[1]
    for q in FOUR:
        if q == 1:
            wait_w(0, 1)
        zp = step_dots(0, q, h0)
        if q == 0:
            for n in EIGHT:
                in_block(0, 2, n, 2 * BLK)
        in_block(0, 1, 2 * q)
        in_block(0, 1, 2 * q + 1)
        if q:
            transpose_rec(0, q // 2, q % 2)
        if q == 1:
            transpose_rec(0, 0, 0)
        h0, c0 = step_gates(0, q, zp, c0)
    wait_w(1, 0)
    wait_w(1, 1)

    def pick(a, b):
        return a + core * (b - a)

    u_b1, u_b2 = pick(mx, rep), pick(rep, mx)
    u_n1 = (pick(rep, flip(rep)), pick(lax.rem(dat + 2, 4), dat))
    u_n2 = (pick(flip(rep), rep), pick(dat, lax.rem(dat + 2, 4)))
    x_core0, y_core1 = (rep, 2 * (flip(mx))), (flip(rep), 2 * mx + 1)
    dests = ((partner, 0, pick(4 + 2 * rep, 2 * mx)), (x_core0, 1 + core, 2 * (flip(mx))), (y_core1, 1 + core, 4 + 2 * (flip(rep))))
    u_col = pick(2 * mx, 4 + 2 * rep)

    def send_h(r0, n):
        for dev, slot, _ in dests:
            remote(hb.at[1, rows(B + r0, n)], hx.at[slot, rows(r0, n)], s_h, v_h, dev).start()

    def send_z(r0, n):
        for dev, slot, c0 in dests:
            remote(dz.at[1, pl.ds(c0, 2), rows(r0, n)], zx.at[slot, :, rows(r0, n)], s_z, v_z, dev).start()

    pl.semaphore_wait(barrier, 7)

    def both(s, carry, last=False):
        h0, c0, h1, c1 = carry
        t0, t1 = 4 * s + 4, 4 * s
        send_h(s * BLK, BLK)
        a = step_dots(0, t0, h0)
        for n in EIGHT:
            in_block(1, s, n)
        h0, c0 = step_gates(0, t0, a, c0)
        for q in FOUR:
            if q < 3:
                a = step_dots(0, t0 + q + 1, h0)
            b = step_dots(1, t1 + q, h1)
            if q < 3:
                h0, c0 = step_gates(0, t0 + q + 1, a, c0)
            transpose_rec(0, 2 * s + 2 + q // 2, q % 2)
            transpose_rec(1, 2 * s + q // 2, q % 2)
            h1, c1 = step_gates(1, t1 + q, b, c1)
            if last and q == MID:
                send_h(6 * 2 * B, 2 * B)
        return h0, c0, h1, c1

    carry = both(0, (h0, c0, None, zero_state[1]))
    carry = both(1, carry)
    h0, c0, h1, c1 = both(2, carry, True)
    send_h(7 * 2 * B, 2 * B)
    for n in EIGHT:
        in_block(1, 3, n)
    for q in FOUR:
        zp = step_dots(1, 12 + q, h1)
        transpose_rec(1, 6 + q // 2, q % 2)
        h1, c1 = step_gates(1, 12 + q, zp, c1)

    pltpu.make_async_copy(dyv, dyv, lsem.at[1]).wait()
    dbacc[...] = jnp.zeros_like(dbacc)

    def bwd_layer(l, e_of, halfway=None, after=None):
        def body(s, carry):
            r, dc_next = carry
            t = T - 1 - s
            r0 = rows(t * B, B)
            i, f, g, o = [gt[l, k, r0, :] for k in FOUR]
            th, c_prev = tc[l, r0, :], cb[l, r0, :]
            dh = e_of(t) + r
            dc = dc_next + dh * o * (1.0 - th * th)
            dzs = (dc * g * i * (1.0 - i), dc * c_prev * f * (1.0 - f), dc * i * (1.0 - g * g), dh * th * o * (1.0 - o))
            acc = None
            for k in ORDER:
                d = dzs[k]
                dbacc[l, :, k * H:(k + 1) * H] += d[0:8] + d[8:SUB] + d[SUB:24] + d[24:32]
                d16 = d.astype(BF16)
                for n in TWO:
                    dz[l, 2 * k + n, r0, :] = d16[:, W * n:W * n + W]
                p = [dot(d16, wt[l, n, pl.ds(k * H, H), :]) for n in TWO]
                acc = p if acc is None else [a + b for a, b in zip(acc, p)]
            return jnp.concatenate(acc, axis=1), dc * f

        zero = jnp.zeros((B, H), F32)
        carry = (zero, zero)
        if after is not None:
            def step_and_send(s, carry):
                carry = body(s, carry)
                after((T - 1 - s) * B)
                return carry
            lax.fori_loop(0, T, step_and_send, carry)
        else:
            carry = lax.fori_loop(0, CUT[0], body, carry)
            halfway(0)
            carry = lax.fori_loop(CUT[0], CUT[1], body, carry)
            halfway(1)
            lax.fori_loop(CUT[1], T, body, carry)

    def dx_of(l, put):
        acc = None
        for m in TWO:
            rr = pl.ds(m * W, W)
            acc = None
            for j in EIGHT:
                p = dot_nt(dz[l, j, rr, :], w[l, 0, j])
                acc = p if acc is None else acc + p
            put(m, acc)

    def block_row(who, q, grp):
        b1 = bits[q][0]
        part = flip(b1) if grp == 0 else b1
        return who * H + q * W + part * BLK

    def cols(half):
        return pl.ds(pl.multiple_of(half * HALF, HALF), HALF)

    def half_of(q, h):
        b2 = bits[q][1]
        return flip(b2) if h == 0 else b2

    def lhs_of(l, who, q, grp):
        r0 = block_row(who, q, grp)
        return hb[l + who, rows(B * (flip(who)), R, B), rows(r0 - who * H, BLK, BLK)].T

    def dw_block(l, who, q, grp, h):
        lt = lhs_of(l, who, q, grp)
        half = half_of(q, h)
        for n in FOUR:
            dwb[l, rows(block_row(who, q, grp), BLK), pl.ds(pl.multiple_of(half * HALF + n * W, W), W)] = (
                dot(lt, dz[l, 4 * half + n]).astype(BF16))

    def cp_rp(l, q, grp, h):
        rr, cc = rows(block_row(flip(core), q, grp), BLK), cols(half_of(q, h))
        return remote(dwb.at[l, rr, cc], rp.at[q, grp, h], s_rp, v_rp.at[grp, h], partner)

    def add_rp(l, q, grp, h):
        r0, cc = block_row(core, q, grp), cols(half_of(q, h))

        @loop(4)
        def _(i):
            rr = rows(r0 + i * 32, 32)
            dwb[l, rr, cc] = (dwb[l, rr, cc].astype(F32) + rp[q, grp, h, rows(i * 32, 32), :].astype(F32)).astype(BF16)

    def place(q, grp, h, i):
        return rows(block_row(core, q, grp) + C * i, C), cols(half_of(q, h))

    def cp_1(l, q, h, i):
        rr, cc = place(q, 0, h, i)
        return remote(dwb.at[l, rr, cc], r1.at[q, h, i], s_1, v_1.at[q, h, i], nbr[q][0])

    def cp_2(l, q, i):
        rr, cc = place(q, 1, 0, i)
        return remote(dwb.at[l, rr, cc], r2.at[q, i], s_2, v_2.at[q, i], nbr[q][1])

    def fin(q, k, i):
        b1, b2 = bits[q]
        c1 = b1 if k in (0, 1) else flip(b1)
        c2 = b2 if k in (0, 2) else flip(b2)
        return rows(core * H + q * W + c1 * BLK + C * i, C), cols(c2)

    def cp_a(l, q, k, i):
        rr, cc = fin(q, 1 if k == 2 else 0, i)
        return remote(res.at[l, rr, cc], res.at[l, rr, cc], s_a, v_a.at[q, k, i], nbr[q][1 if k == 0 else 0])

    def cp_p(l, q, k, i):
        rr, cc = fin(q, k, i)
        return remote(res.at[l, rr, cc], res.at[l, rr, cc], s_p, v_p, partner)

    QI = [(q, i) for i in TWO for q in TWO]

    def dw_pair(l, who, grp, h):
        for q in TWO:
            dw_block(l, who, q, grp, h)
            if who is not core:
                cp_rp(l, q, grp, h).start()

    def take_rp(l, grp, h):
        pair = rp.at[:, grp, h]
        remote(pair, pair, s_rp, v_rp.at[grp, h], partner).wait_recv()
        for q in TWO:
            add_rp(l, q, grp, h)
            if grp == 0:
                for i in TWO:
                    cp_1(l, q, h, i).start()

    def grads_send(l):
        other = flip(core)
        dw_pair(l, other, 0, 0)
        dw_pair(l, core, 0, 0)
        dw_pair(l, other, 0, 1)
        take_rp(l, 0, 0)
        dw_pair(l, core, 0, 1)
        dw_pair(l, other, 1, 0)
        take_rp(l, 0, 1)
        dw_pair(l, core, 1, 0)
        dw_pair(l, other, 1, 1)
        dw_pair(l, core, 1, 1)

    def recv_1(l, h):
        if h == 0:
            take_rp(l, 1, 0)
            take_rp(l, 1, 1)
        for q, i in QI:
            cp_1(l, q, h, i).wait_recv()
            rr, cc = place(q, 1, h, i)
            dwb[l, rr, cc] = (dwb[l, rr, cc].astype(F32) + r1[q, h, i].astype(F32)).astype(BF16)
            if h == 0:
                cp_2(l, q, i).start()

    def recv_2(l):
        for q, i in QI:
            cp_2(l, q, i).wait_recv()
            rr, cc = fin(q, 0, i)
            res[l, rr, cc] = (dwb[l, rr, cc].astype(F32) + r2[q, i].astype(F32)).astype(BF16)
            cp_a(l, q, 0, i).start()
            cp_p(l, q, 0, i).start()

    def send_a1(l):
        for q, i in QI:
            cp_a(l, q, 1, i).start()

    def recv_a1(l):
        for q, i in QI:
            cp_a(l, q, 0, i).wait_recv()
            cp_a(l, q, 2, i).start()
            cp_p(l, q, 1, i).start()

    def recv_a2(l, k):
        for q, i in QI:
            cp_a(l, q, k, i).wait_recv()
            cp_p(l, q, k + 1, i).start()

    def h_row(who, q):
        return H + who * W + q * BLK

    def dwh_block(who, q, grp):
        lt = hb[2, pl.ds(0, R), rows(h_row(who, q) - H, BLK, BLK)].T
        half = flip(bits[q][0]) if grp == 0 else bits[q][0]
        for n in FOUR:
            dwb[1, rows(h_row(who, q), BLK), pl.ds(pl.multiple_of(half * HALF + n * W, W), W)] = (
                dot(lt, dz[1, 4 * half + n]).astype(BF16))

    def cp_rph(q, grp):
        half = flip(bits[q][0]) if grp == 0 else bits[q][0]
        return remote(dwb.at[1, rows(h_row(flip(core), q), BLK), cols(half)], rph.at[q, grp], s_rph, v_rph.at[grp], partner)

    def quarter(q, grp, h):
        half = flip(bits[q][0]) if grp == 0 else bits[q][0]
        return pl.ds(pl.multiple_of(half * HALF + QTR * half_of(q, h), QTR), QTR)

    def cp_1h(q, h):
        return remote(dwb.at[1, rows(h_row(core, q), BLK), quarter(q, 0, h)], r1h.at[q, h], s_1h, v_1h.at[q, h], nbr[q][0])

    def take_rph(grp):
        pair = rph.at[:, grp]
        remote(pair, pair, s_rph, v_rph.at[grp], partner).wait_recv()
        for q in TWO:
            r0, cc = h_row(core, q), cols(flip(bits[q][0]) if grp == 0 else bits[q][0])

            @loop(4)
            def _(i):
                rr = rows(r0 + i * 32, 32)
                dwb[1, rr, cc] = (dwb[1, rr, cc].astype(F32) + rph[q, grp, rows(i * 32, 32), :].astype(F32)).astype(BF16)
            if grp == 0:
                for h in TWO:
                    cp_1h(q, h).start()

    def grads_send_1():
        for grp in TWO:
            for q in TWO:
                dwh_block(flip(core), q, grp)
                cp_rph(q, grp).start()
            for q in TWO:
                dwh_block(core, q, grp)
            if grp == 0:
                take_rph(0)

    def sum_u():
        remote(hx, hx, s_h, v_h, partner).wait_recv()
        remote(zx, zx, s_z, v_z, partner).wait_recv()
        for m in FOUR:
            f0 = pl.ds(m * BLK, BLK)
            lts = [hb[1, pl.ds(B, R), f0].T] + [hx[i, :, f0].T for i in THREE]
            for n in TWO:
                zs = [dz[1, u_col + n]] + [zx[i, n] for i in THREE]
                acc = None
                for lt, z in zip(lts, zs):
                    p = dot(lt, z).astype(BF16).astype(F32)
                    acc = p if acc is None else acc + p
                ub[f0, W * n:W * n + W] = acc.astype(BF16)

    def item_nbr(j):
        return (u_n1, u_n2) if j < 2 else nbr[j - 2]

    def item_fin(j, k):
        b1, b2 = (u_b1, u_b2) if j < 2 else bits[j - 2]
        c1 = b1 if k in (0, 1) else flip(b1)
        c2 = b2 if k in (0, 2) else flip(b2)
        if j < 2:
            return rows(W * c2 + BLK * j, BLK), pl.ds(pl.multiple_of(core * HALF + QTR * c1, QTR), QTR)
        return rows(h_row(core, j - 2), BLK), pl.ds(pl.multiple_of(HALF * c1 + QTR * c2, QTR), QTR)

    def cp_2x(j):
        if j < 2:
            src, dst = ub.at[rows(W * (flip(u_b2)) + BLK * j, BLK)], r2u.at[j]
        else:
            src, dst = dwb.at[1, rows(h_row(core, j - 2), BLK), quarter(j - 2, 1, 0)], r2h.at[j - 2]
        return remote(src, dst, s_2x, v_2x.at[j], item_nbr(j)[1])

    def cp_ax(j, k):
        rr, cc = item_fin(j, 1 if k == 2 else 0)
        return remote(res.at[1, rr, cc], res.at[1, rr, cc], s_ax, v_ax.at[j if k == 0 else 3 + k], item_nbr(j)[1 if k == 0 else 0])

    def cp_px(j, k):
        rr, cc = item_fin(j, k)
        return remote(res.at[1, rr, cc], res.at[1, rr, cc], s_px, v_px, partner)

    JS = (2, 3, 0, 1)

    def recv_1h(h):
        if h == 0:
            take_rph(1)
        for q in TWO:
            cp_1h(q, h).wait_recv()
            rr, cc = rows(h_row(core, q), BLK), quarter(q, 1, h)
            dwb[1, rr, cc] = (dwb[1, rr, cc].astype(F32) + r1h[q, h].astype(F32)).astype(BF16)
            if h == 0:
                cp_2x(2 + q).start()

    def recv_2x():
        for j in JS:
            cp_2x(j).wait_recv()
            rr, cc = item_fin(j, 0)
            if j < 2:
                mine, got = ub[rows(W * u_b2 + BLK * j, BLK), :], r2u[j]
            else:
                mine, got = dwb[1, rr, cc], r2h[j - 2]
            res[1, rr, cc] = (mine.astype(F32) + got.astype(F32)).astype(BF16)
            cp_ax(j, 0).start()
            cp_px(j, 0).start()

    def send_a1x():
        for j in JS:
            cp_ax(j, 1).start()

    def recv_a1x():
        for j in JS:
            cp_ax(j, 0).wait_recv()
            cp_ax(j, 2).start()
            cp_px(j, 1).start()

    def recv_a2x(k):
        part = res.at[1, pl.ds(0, BLK)]
        remote(part, part, s_ax, v_ax.at[3 + k], partner).wait_recv()
        for j in JS:
            cp_px(j, k + 1).start()

    def between(part):
        if part == 0:
            sum_u()
            for j in TWO:
                cp_2x(j).start()
        else:
            recv_1h(0)

    bwd_layer(1, lambda t: jnp.concatenate([dyv[k, pl.ds(t, B, stride=T), :] for k in FOUR], axis=1), after=lambda r0: send_z(r0, B))
    grads_send_1()

    def put_e(m, v):
        eb[pl.ds(m * W, W), :] = v
    dx_of(1, put_e)
    bwd_layer(0, lambda t: eb[rows(t * B, B), :], between)
    grads_send(0)

    for l in TWO:
        for j in EIGHT:
            dbs[8 * l + j:8 * l + j + 1, :] = jnp.sum(dbacc[l, :, W * j:W * j + W], axis=0, keepdims=True)
    dbb[...] = dbs[...].astype(BF16)
    me = rep * 4 + dat
    cps = [remote(dbb, dbr.at[d - 1], s_db, v_db, dev) for d, dev in enumerate(others, 1)]
    for c in cps:
        c.start()

    def put_dx(m, v):
        for s in EIGHT:
            for k in FOUR:
                dxo[k, pl.ds(8 * m + s, B, stride=T), :] = v[s * B:(s + 1) * B, k * BLK:(k + 1) * BLK]

    recv_1h(1)
    recv_2x()
    dx_of(0, put_dx)
    recv_1(0, 0)
    send_a1x()
    recv_1(0, 1)
    recv_a1x()
    recv_2(0)
    send_a1(0)
    recv_a2x(1)
    recv_a2x(2)
    remote(dbr, dbr, s_db, v_db, partner).wait_recv()
    tot = dbb[...].astype(F32)
    for d in range(7):
        tot += dbr[d].astype(F32)
    dbo[...] = tot
    recv_a1(0)
    recv_a2(0, 1)
    recv_a2(0, 2)
    for n, sem in ((QTR, s_rp), (W, s_1), (BLK, s_2), (384, s_a), (W, s_rph), (BLK, s_1h), (BLK, s_2x), (384, s_ax)):
        part = dwb.at[0, pl.ds(0, n)]
        remote(part, part, sem, v_p, partner).wait_send()
    remote(hx, hx, s_h, v_p, partner).wait_send()
    remote(zx, zx, s_z, v_p, partner).wait_send()
    for l, snd, rcv in ((0, s_p, v_p), (1, s_px, v_px)):
        half_w = res.at[l, pl.ds(0, H)]
        remote(half_w, half_w, snd, rcv, partner).wait()
    remote(dbr, dbr, s_db, v_db, partner).wait_send()


def out_kernel(res, dbo, dxo, dw_ref, db_ref, dx_ref, buf, dbv, sem, xsem):
    cx = [pltpu.make_async_copy(dxo.at[k], dx_ref.at[:, pl.ds(k * BLK, BLK)], xsem.at[k]) for k in FOUR]
    for l in TWO:
        for j in EIGHT:
            dbv[l:l + 1, W * j:W * j + W] = dbo[8 * l + j:8 * l + j + 1, :]
    cx.append(pltpu.make_async_copy(dbv, db_ref, xsem.at[4]))
    for c in cx:
        c.start()
    n = 64

    def cp(s):
        return pltpu.make_async_copy(buf.at[s], dw_ref.at[s // SUB, rows(lax.rem(s, SUB) * n, n)], sem)

    @loop(32)
    def _(s):
        buf[s] = res[s // SUB, rows(lax.rem(s, SUB) * n, n), :].astype(F32)
        cp(s).start()

    pltpu.make_async_copy(buf, buf, sem).wait()
    for c in cx:
        c.wait()


def solution(mesh):
    vm = pl.BlockSpec(memory_space=pltpu.VMEM)
    hbm = pl.BlockSpec(memory_space=pl.ANY)
    dma, vmem = pltpu.SemaphoreType.DMA, pltpu.VMEM

    def local_step(x, dy, w, b):
        scratch = [
            vmem((2, G), F32),
            vmem((4, R, BLK), BF16), vmem((4, B * PAD, BLK), F32), vmem((4, R, BLK), F32),
            vmem((2, 2, 8, H, W), BF16), vmem((2, 2, G, W), BF16), vmem((3, R + B, H), BF16),
            vmem((2, 4, R, H), F32), vmem((2, R + B, H), F32), vmem((2, R, H), F32),
            vmem((2, 8, R, W), BF16), vmem((R, H), F32), vmem((2, 8, G), F32),
            vmem((SUB, W), F32), vmem((SUB, W), BF16), vmem((7, SUB, W), BF16),
            vmem((2, 2 * H, G), BF16), vmem(P3 + (BLK, HALF), BF16),
            vmem(P3 + (C, HALF), BF16), vmem(P2 + (C, HALF), BF16),
            vmem((3, R, H), BF16), vmem((3, 2, R, W), BF16), vmem((H, QTR), BF16),
            vmem(P2 + (BLK, HALF), BF16), vmem(P2 + (BLK, QTR), BF16), vmem((2, BLK, QTR), BF16),
            vmem((2, BLK, QTR), BF16),
            dma((7,)), dma, dma(P2), dma, dma(P3), dma, dma(P2), dma, dma((2, 3, 2)), dma, dma, dma, dma,
            dma, dma, dma, dma, dma, dma((2,)), dma, dma(P2), dma, dma((4,)), dma, dma((6,)), dma, dma,
        ]
        res, dbo, dxo = pl.pallas_call(
            step_kernel,
            out_shape=(vmem((2, 2 * H, G), BF16), vmem((SUB, W), F32), vmem((4, R, BLK), F32)),
            in_specs=[hbm, hbm, hbm, hbm], out_specs=(vm, vm, vm), scratch_shapes=scratch,
            compiler_params=pltpu.CompilerParams(collective_id=0, has_side_effects=True, vmem_limit_bytes=VMEM_LIMIT),
        )(x.reshape(R, H), dy.reshape(R, H), w, b)
        dw, db, dx = pl.pallas_call(
            out_kernel,
            out_shape=(jax.ShapeDtypeStruct((2, 2 * H, G), F32), jax.ShapeDtypeStruct((2, G), F32),
                       jax.ShapeDtypeStruct((R, H), F32)),
            in_specs=[vm, vm, vm], out_specs=(hbm, hbm, hbm),
            scratch_shapes=[vmem((32, 64, G), F32), vmem((2, G), F32), dma, dma((5,))],
            compiler_params=pltpu.CompilerParams(vmem_limit_bytes=32 * HALF * HALF),
        )(res, dbo, dxo)
        return dw, db, dx.reshape(B, T, H)

    rows_spec = P(("replica", "data"))
    return jax.shard_map(local_step, mesh=mesh, in_specs=(rows_spec, rows_spec, P(), P()),
                         out_specs=(P(), P(), rows_spec), check_vma=False)
```

```python
import jax
import jax.numpy as jnp
from jax import lax
from jax.experimental import pallas as pl
from jax.experimental.pallas import tpu as pltpu
from jax.sharding import PartitionSpec as P

F32, BF16 = jnp.float32, jnp.bfloat16
MESH = pl.DeviceIdType.MESH
T, B, H = 16, 32, 512
G, R = 4 * H, T * B
ORDER = (0, 1, 2, 3)
PAD = 24
MID = 2
CUT = (6, 13)
TWO, THREE, FOUR, EIGHT = range(2), range(3), range(4), range(8)
W = 256
BLK, QTR, HALF, SUB = 128, 512, 1024, 16
P2, P3 = (2, 2), (2, 2, 2)
VMEM_LIMIT = 54 * 1024 * 1024
C = 64


def flip(bit):
    return 1 - bit


def loop(n):
    return pl.loop(0, n)


def dot(a, b):
    return jnp.dot(a, b, preferred_element_type=F32)


def dot_k(a, b, k):
    acc = None
    for i in range(0, a.shape[1], k):
        p = dot(a[:, i:i + k], b[i:i + k])
        acc = p if acc is None else acc + p
    return acc


def dot_nt(a, b):
    return lax.dot_general(a, b, (((1,), (1,)), ((), ())), preferred_element_type=F32)


def sigmoid(z):
    return 0.5 * jnp.tanh(0.5 * z) + 0.5


def rows(start, n, m=SUB):
    return pl.ds(start, n) if isinstance(start, int) else pl.ds(pl.multiple_of(start, m), n)


def step_kernel(x_hbm, dy_hbm, w_hbm, b_hbm, res, dbo, dxo,
                b_ref, xv, xf, dyv, w, wt, hb, gt, cb, tc, dz, eb, dbacc, dbs, dbb, dbr, dwb, rp, r1, r2,
                hx, zx, ub, rph, r1h, r2u, r2h,
                lsem, s_rp, v_rp, s_1, v_1, s_2, v_2, s_a, v_a, s_p, v_p, s_db, v_db,
                s_h, v_h, s_z, v_z, s_rph, v_rph, s_1h, v_1h, s_2x, v_2x, s_ax, v_ax, s_px, v_px):
    rep = lax.axis_index("replica")
    dat = lax.axis_index("data")
    mx, core = dat // 2, dat % 2
    partner = (rep, dat + 1 - 2 * core)
    x_nbr = (rep, lax.rem(dat + 2, 4))
    y_nbr = (flip(rep), dat)
    nbr = ((x_nbr, y_nbr), (y_nbr, x_nbr))
    bits = ((mx, rep), (rep, mx))

    def remote(src, dst, s, v, dev):
        return pltpu.make_async_remote_copy(src_ref=src, dst_ref=dst, send_sem=s, recv_sem=v,
                                            device_id=dev, device_id_type=MESH)

    others = [(lax.rem(rep + (d // 4), 2), lax.rem(dat + (d % 4), 4)) for d in range(1, 8)]
    barrier = pltpu.get_barrier_semaphore()

    ld_x = [pltpu.make_async_copy(x_hbm.at[:, pl.ds(k * BLK, BLK)], xv.at[k], lsem.at[0]) for k in FOUR]
    ld_dy = [pltpu.make_async_copy(dy_hbm.at[:, pl.ds(k * BLK, BLK)], dyv.at[k], lsem.at[1]) for k in FOUR]
    ld_w = [pltpu.make_async_copy(w_hbm.at[l, pl.ds(k * H, H), pl.ds(j * W, W)], w.at[l, k, j],
                                  lsem.at[2 + 2 * l + k])
            for l in TWO for k in TWO for j in EIGHT]
    ld_b = pltpu.make_async_copy(b_hbm, b_ref, lsem.at[6])
    for c in ld_x + [ld_b] + ld_w[:8]:
        c.start()
    for dev in others:
        pl.semaphore_signal(barrier, inc=1, device_id=dev, device_id_type=MESH)
    for l in TWO:
        hb[l + 1, pl.ds(0, B), :] = jnp.zeros((B, H), BF16)
        cb[l, pl.ds(0, B), :] = jnp.zeros((B, H), F32)
    pltpu.make_async_copy(xv, xv, lsem.at[0]).wait()
    for c in ld_w[8:SUB]:
        c.start()
    for i in range(B):
        xf[:, i * PAD:i * PAD + T, :] = xv[:, i * T:(i + 1) * T, :].astype(F32)

    @loop(T)
    def _(t):
        hb[0, rows((t + 1) * B, B), :] = jnp.concatenate(
            [xf[k, pl.ds(t, B, stride=PAD), :] for k in FOUR], axis=1).astype(BF16)
    for c in ld_w[SUB:] + ld_dy:
        c.start()

    def wait_w(l, k):
        pltpu.make_async_copy(w.at[l, k], w.at[l, k], lsem.at[2 + 2 * l + k]).wait()

    ld_b.wait()
    pltpu.make_async_copy(w.at[0, 0], w.at[0, 0], lsem.at[2]).wait()

    def in_block(l, s, n, m=BLK):
        r0 = rows(s * BLK, m)
        gt[l, n // 2, r0, W * (n % 2):W * (n % 2) + W] = (
            dot(hb[l, rows(B + s * BLK, m), :], w[l, 0, n]) + b_ref[l:l + 1, W * n:W * n + W])

    def transpose_rec(l, j, n):
        wt[l, n, rows(j * W, W), :] = w[l, 1, j, pl.ds(n * W, W), :].T

    def step_dots(l, t, h):
        zin = [gt[l, k, rows(t * B, B), :] for k in FOUR]
        prod = [None] * 8
        if h is None:
            return zin, prod
        for k in (0, 2, 1, 3):
            for n in TWO:
                prod[2 * k + n] = dot_k(h, w[l, 1, 2 * k + n], BLK)
        return zin, prod

    def step_gates(l, t, zp, c):
        zin, prod = zp
        r0, r1_ = rows(t * B, B), rows((t + 1) * B, B)
        hs, cs = [], []
        for n in TWO:
            m = slice(W * n, W * n + W)
            z = [zin[k][:, m] if prod[2 * k + n] is None else zin[k][:, m] + prod[2 * k + n] for k in FOUR]
            i, g, f, o = sigmoid(z[0]), jnp.tanh(z[2]), sigmoid(z[1]), sigmoid(z[3])
            cn = f * c[:, m] + i * g
            th = jnp.tanh(cn)
            hn = (o * th).astype(BF16)
            for k, v in enumerate((i, f, g, o)):
                gt[l, k, r0, m] = v
            cb[l, r1_, m] = cn
            tc[l, r0, m] = th
            hb[l + 1, r1_, m] = hn
            hs.append(hn)
            cs.append(cn)
        return jnp.concatenate(hs, axis=1), jnp.concatenate(cs, axis=1)

    zero_state = (jnp.zeros((B, H), BF16), jnp.zeros((B, H), F32))
    for n in EIGHT:
        in_block(0, 0, n)
    h0, c0 = None, zero_state[1]
    for q in FOUR:
        if q == 1:
            wait_w(0, 1)
        zp = step_dots(0, q, h0)
        if q == 0:
            for n in EIGHT:
                in_block(0, 2, n, 2 * BLK)
        in_block(0, 1, 2 * q)
        in_block(0, 1, 2 * q + 1)
        if q:
            transpose_rec(0, q // 2, q % 2)
        if q == 1:
            transpose_rec(0, 0, 0)
        h0, c0 = step_gates(0, q, zp, c0)
    wait_w(1, 0)
    wait_w(1, 1)

    def pick(a, b):
        return a + core * (b - a)

    u_b1, u_b2 = pick(mx, rep), pick(rep, mx)
    u_n1 = (pick(rep, flip(rep)), pick(lax.rem(dat + 2, 4), dat))
    u_n2 = (pick(flip(rep), rep), pick(dat, lax.rem(dat + 2, 4)))
    x_core0, y_core1 = (rep, 2 * (flip(mx))), (flip(rep), 2 * mx + 1)
    dests = ((partner, 0, pick(4 + 2 * rep, 2 * mx)), (x_core0, 1 + core, 2 * (flip(mx))), (y_core1, 1 + core, 4 + 2 * (flip(rep))))
    u_col = pick(2 * mx, 4 + 2 * rep)

    def send_h(r0, n):
        for dev, slot, _ in dests:
            remote(hb.at[1, rows(B + r0, n)], hx.at[slot, rows(r0, n)], s_h, v_h, dev).start()

    def send_z(r0, n):
        for dev, slot, c0 in dests:
            remote(dz.at[1, pl.ds(c0, 2), rows(r0, n)], zx.at[slot, :, rows(r0, n)], s_z, v_z, dev).start()

    pl.semaphore_wait(barrier, 7)

    def both(s, carry, last=False):
        h0, c0, h1, c1 = carry
        t0, t1 = 4 * s + 4, 4 * s
        send_h(s * BLK, BLK)
        a = step_dots(0, t0, h0)
        for n in EIGHT:
            in_block(1, s, n)
        h0, c0 = step_gates(0, t0, a, c0)
        for q in FOUR:
            if q < 3:
                a = step_dots(0, t0 + q + 1, h0)
            b = step_dots(1, t1 + q, h1)
            if q < 3:
                h0, c0 = step_gates(0, t0 + q + 1, a, c0)
            transpose_rec(0, 2 * s + 2 + q // 2, q % 2)
            transpose_rec(1, 2 * s + q // 2, q % 2)
            h1, c1 = step_gates(1, t1 + q, b, c1)
            if last and q == MID:
                send_h(6 * 2 * B, 2 * B)
        return h0, c0, h1, c1

    carry = both(0, (h0, c0, None, zero_state[1]))
    carry = both(1, carry)
    h0, c0, h1, c1 = both(2, carry, True)
    send_h(7 * 2 * B, 2 * B)
    for q in FOUR:
        zp = step_dots(1, 12 + q, h1)
        if q == 0:
            for n in EIGHT:
                in_block(1, 3, n)
            zp = [gt[1, k, rows(12 * B, B), :] for k in FOUR], zp[1]
        transpose_rec(1, 6 + q // 2, q % 2)
        h1, c1 = step_gates(1, 12 + q, zp, c1)

    pltpu.make_async_copy(dyv, dyv, lsem.at[1]).wait()
    dbacc[...] = jnp.zeros_like(dbacc)

    def bwd_layer(l, e_of, halfway=None, after=None):
        def body(s, carry):
            r, dc_next = carry
            t = T - 1 - s
            r0 = rows(t * B, B)
            i, f, g, o = [gt[l, k, r0, :] for k in FOUR]
            th, c_prev = tc[l, r0, :], cb[l, r0, :]
            dh = e_of(t) + r
            dc = dc_next + dh * o * (1.0 - th * th)
            dzs = (dc * g * i * (1.0 - i), dc * c_prev * f * (1.0 - f), dc * i * (1.0 - g * g), dh * th * o * (1.0 - o))
            acc = None
            for k in ORDER:
                d = dzs[k]
                dbacc[l, :, k * H:(k + 1) * H] += d[0:8] + d[8:SUB] + d[SUB:24] + d[24:32]
                d16 = d.astype(BF16)
                for n in TWO:
                    dz[l, 2 * k + n, r0, :] = d16[:, W * n:W * n + W]
                p = [dot_k(d16, wt[l, n, pl.ds(k * H, H), :], BLK) for n in TWO]
                acc = p if acc is None else [a + b for a, b in zip(acc, p)]
            return jnp.concatenate(acc, axis=1), dc * f

        zero = jnp.zeros((B, H), F32)
        carry = (zero, zero)
        if after is not None:
            def step_and_send(s, carry):
                carry = body(s, carry)
                after((T - 1 - s) * B)
                return carry
            lax.fori_loop(0, T, step_and_send, carry)
        else:
            carry = lax.fori_loop(0, CUT[0], body, carry)
            halfway(0)
            carry = lax.fori_loop(CUT[0], CUT[1], body, carry)
            halfway(1)
            lax.fori_loop(CUT[1], T, body, carry)

    def dx_of(l, put):
        acc = None
        for m in TWO:
            rr = pl.ds(m * W, W)
            acc = None
            for j in EIGHT:
                p = dot_nt(dz[l, j, rr, :], w[l, 0, j])
                acc = p if acc is None else acc + p
            put(m, acc)

    def block_row(who, q, grp):
        b1 = bits[q][0]
        part = flip(b1) if grp == 0 else b1
        return who * H + q * W + part * BLK

    def cols(half):
        return pl.ds(pl.multiple_of(half * HALF, HALF), HALF)

    def half_of(q, h):
        b2 = bits[q][1]
        return flip(b2) if h == 0 else b2

    def lhs_of(l, who, q, grp):
        r0 = block_row(who, q, grp)
        return hb[l + who, rows(B * (flip(who)), R, B), rows(r0 - who * H, BLK, BLK)].T

    def dw_block(l, who, q, grp, h):
        lt = lhs_of(l, who, q, grp)
        half = half_of(q, h)
        for n in FOUR:
            dwb[l, rows(block_row(who, q, grp), BLK), pl.ds(pl.multiple_of(half * HALF + n * W, W), W)] = (
                dot(lt, dz[l, 4 * half + n]).astype(BF16))

    def cp_rp(l, q, grp, h):
        rr, cc = rows(block_row(flip(core), q, grp), BLK), cols(half_of(q, h))
        return remote(dwb.at[l, rr, cc], rp.at[q, grp, h], s_rp, v_rp.at[grp, h], partner)

    def add_rp(l, q, grp, h):
        r0, cc = block_row(core, q, grp), cols(half_of(q, h))

        @loop(4)
        def _(i):
            rr = rows(r0 + i * 32, 32)
            dwb[l, rr, cc] = (dwb[l, rr, cc].astype(F32) + rp[q, grp, h, rows(i * 32, 32), :].astype(F32)).astype(BF16)

    def place(q, grp, h, i):
        return rows(block_row(core, q, grp) + C * i, C), cols(half_of(q, h))

    def cp_1(l, q, h, i):
        rr, cc = place(q, 0, h, i)
        return remote(dwb.at[l, rr, cc], r1.at[q, h, i], s_1, v_1.at[q, h, i], nbr[q][0])

    def cp_2(l, q, i):
        rr, cc = place(q, 1, 0, i)
        return remote(dwb.at[l, rr, cc], r2.at[q, i], s_2, v_2.at[q, i], nbr[q][1])

    def fin(q, k, i):
        b1, b2 = bits[q]
        c1 = b1 if k in (0, 1) else flip(b1)
        c2 = b2 if k in (0, 2) else flip(b2)
        return rows(core * H + q * W + c1 * BLK + C * i, C), cols(c2)

    def cp_a(l, q, k, i):
        rr, cc = fin(q, 1 if k == 2 else 0, i)
        return remote(res.at[l, rr, cc], res.at[l, rr, cc], s_a, v_a.at[q, k, i], nbr[q][1 if k == 0 else 0])

    def cp_p(l, q, k, i):
        rr, cc = fin(q, k, i)
        return remote(res.at[l, rr, cc], res.at[l, rr, cc], s_p, v_p, partner)

    QI = [(q, i) for i in TWO for q in TWO]

    def dw_pair(l, who, grp, h):
        for q in TWO:
            dw_block(l, who, q, grp, h)
            if who is not core:
                cp_rp(l, q, grp, h).start()

    def take_rp(l, grp, h):
        pair = rp.at[:, grp, h]
        remote(pair, pair, s_rp, v_rp.at[grp, h], partner).wait_recv()
        for q in TWO:
            add_rp(l, q, grp, h)
            if grp == 0:
                for i in TWO:
                    cp_1(l, q, h, i).start()

    def grads_send(l):
        other = flip(core)
        dw_pair(l, other, 0, 0)
        dw_pair(l, core, 0, 0)
        dw_pair(l, other, 0, 1)
        take_rp(l, 0, 0)
        dw_pair(l, core, 0, 1)
        dw_pair(l, other, 1, 0)
        take_rp(l, 0, 1)
        dw_pair(l, core, 1, 0)
        dw_pair(l, other, 1, 1)
        dw_pair(l, core, 1, 1)

    def recv_1(l, h):
        if h == 0:
            take_rp(l, 1, 0)
            take_rp(l, 1, 1)
        for q, i in QI:
            cp_1(l, q, h, i).wait_recv()
            rr, cc = place(q, 1, h, i)
            dwb[l, rr, cc] = (dwb[l, rr, cc].astype(F32) + r1[q, h, i].astype(F32)).astype(BF16)
            if h == 0:
                cp_2(l, q, i).start()

    def recv_2(l):
        for q, i in QI:
            cp_2(l, q, i).wait_recv()
            rr, cc = fin(q, 0, i)
            res[l, rr, cc] = (dwb[l, rr, cc].astype(F32) + r2[q, i].astype(F32)).astype(BF16)
            cp_a(l, q, 0, i).start()
            cp_p(l, q, 0, i).start()

    def send_a1(l):
        for q, i in QI:
            cp_a(l, q, 1, i).start()

    def recv_a1(l):
        for q, i in QI:
            cp_a(l, q, 0, i).wait_recv()
            cp_a(l, q, 2, i).start()
            cp_p(l, q, 1, i).start()

    def recv_a2(l, k):
        for q, i in QI:
            cp_a(l, q, k, i).wait_recv()
            cp_p(l, q, k + 1, i).start()

    def h_row(who, q):
        return H + who * W + q * BLK

    def dwh_block(who, q, grp):
        lt = hb[2, pl.ds(0, R), rows(h_row(who, q) - H, BLK, BLK)].T
        half = flip(bits[q][0]) if grp == 0 else bits[q][0]
        for n in FOUR:
            dwb[1, rows(h_row(who, q), BLK), pl.ds(pl.multiple_of(half * HALF + n * W, W), W)] = (
                dot(lt, dz[1, 4 * half + n]).astype(BF16))

    def cp_rph(q, grp):
        half = flip(bits[q][0]) if grp == 0 else bits[q][0]
        return remote(dwb.at[1, rows(h_row(flip(core), q), BLK), cols(half)], rph.at[q, grp], s_rph, v_rph.at[grp], partner)

    def quarter(q, grp, h):
        half = flip(bits[q][0]) if grp == 0 else bits[q][0]
        return pl.ds(pl.multiple_of(half * HALF + QTR * half_of(q, h), QTR), QTR)

    def cp_1h(q, h):
        return remote(dwb.at[1, rows(h_row(core, q), BLK), quarter(q, 0, h)], r1h.at[q, h], s_1h, v_1h.at[q, h], nbr[q][0])

    def take_rph(grp):
        pair = rph.at[:, grp]
        remote(pair, pair, s_rph, v_rph.at[grp], partner).wait_recv()
        for q in TWO:
            r0, cc = h_row(core, q), cols(flip(bits[q][0]) if grp == 0 else bits[q][0])

            @loop(4)
            def _(i):
                rr = rows(r0 + i * 32, 32)
                dwb[1, rr, cc] = (dwb[1, rr, cc].astype(F32) + rph[q, grp, rows(i * 32, 32), :].astype(F32)).astype(BF16)
            if grp == 0:
                for h in TWO:
                    cp_1h(q, h).start()

    def grads_send_1():
        for grp in TWO:
            for q in TWO:
                dwh_block(flip(core), q, grp)
                cp_rph(q, grp).start()
            for q in TWO:
                dwh_block(core, q, grp)
            if grp == 0:
                take_rph(0)

    def sum_u():
        remote(hx, hx, s_h, v_h, partner).wait_recv()
        remote(zx, zx, s_z, v_z, partner).wait_recv()
        for m in FOUR:
            f0 = pl.ds(m * BLK, BLK)
            lts = [hb[1, pl.ds(B, R), f0].T] + [hx[i, :, f0].T for i in THREE]
            for n in TWO:
                zs = [dz[1, u_col + n]] + [zx[i, n] for i in THREE]
                acc = None
                for lt, z in zip(lts, zs):
                    p = dot(lt, z).astype(BF16).astype(F32)
                    acc = p if acc is None else acc + p
                ub[f0, W * n:W * n + W] = acc.astype(BF16)

    def item_nbr(j):
        return (u_n1, u_n2) if j < 2 else nbr[j - 2]

    def item_fin(j, k):
        b1, b2 = (u_b1, u_b2) if j < 2 else bits[j - 2]
        c1 = b1 if k in (0, 1) else flip(b1)
        c2 = b2 if k in (0, 2) else flip(b2)
        if j < 2:
            return rows(W * c2 + BLK * j, BLK), pl.ds(pl.multiple_of(core * HALF + QTR * c1, QTR), QTR)
        return rows(h_row(core, j - 2), BLK), pl.ds(pl.multiple_of(HALF * c1 + QTR * c2, QTR), QTR)

    def cp_2x(j):
        if j < 2:
            src, dst = ub.at[rows(W * (flip(u_b2)) + BLK * j, BLK)], r2u.at[j]
        else:
            src, dst = dwb.at[1, rows(h_row(core, j - 2), BLK), quarter(j - 2, 1, 0)], r2h.at[j - 2]
        return remote(src, dst, s_2x, v_2x.at[j], item_nbr(j)[1])

    def cp_ax(j, k):
        rr, cc = item_fin(j, 1 if k == 2 else 0)
        return remote(res.at[1, rr, cc], res.at[1, rr, cc], s_ax, v_ax.at[j if k == 0 else 3 + k], item_nbr(j)[1 if k == 0 else 0])

    def cp_px(j, k):
        rr, cc = item_fin(j, k)
        return remote(res.at[1, rr, cc], res.at[1, rr, cc], s_px, v_px, partner)

    JS = (2, 3, 0, 1)

    def recv_1h(h):
        if h == 0:
            take_rph(1)
        for q in TWO:
            cp_1h(q, h).wait_recv()
            rr, cc = rows(h_row(core, q), BLK), quarter(q, 1, h)
            dwb[1, rr, cc] = (dwb[1, rr, cc].astype(F32) + r1h[q, h].astype(F32)).astype(BF16)
            if h == 0:
                cp_2x(2 + q).start()

    def recv_2x():
        for j in JS:
            cp_2x(j).wait_recv()
            rr, cc = item_fin(j, 0)
            if j < 2:
                mine, got = ub[rows(W * u_b2 + BLK * j, BLK), :], r2u[j]
            else:
                mine, got = dwb[1, rr, cc], r2h[j - 2]
            res[1, rr, cc] = (mine.astype(F32) + got.astype(F32)).astype(BF16)
            cp_ax(j, 0).start()
            cp_px(j, 0).start()

    def send_a1x():
        for j in JS:
            cp_ax(j, 1).start()

    def recv_a1x():
        for j in JS:
            cp_ax(j, 0).wait_recv()
            cp_ax(j, 2).start()
            cp_px(j, 1).start()

    def recv_a2x(k):
        part = res.at[1, pl.ds(0, BLK)]
        remote(part, part, s_ax, v_ax.at[3 + k], partner).wait_recv()
        for j in JS:
            cp_px(j, k + 1).start()

    def between(part):
        if part == 0:
            sum_u()
            for j in TWO:
                cp_2x(j).start()
        else:
            recv_1h(0)

    bwd_layer(1, lambda t: jnp.concatenate([dyv[k, pl.ds(t, B, stride=T), :] for k in FOUR], axis=1), after=lambda r0: send_z(r0, B))
    grads_send_1()

    def put_e(m, v):
        eb[pl.ds(m * W, W), :] = v
    dx_of(1, put_e)
    bwd_layer(0, lambda t: eb[rows(t * B, B), :], between)
    grads_send(0)

    for l in TWO:
        for j in EIGHT:
            dbs[8 * l + j:8 * l + j + 1, :] = jnp.sum(dbacc[l, :, W * j:W * j + W], axis=0, keepdims=True)
    dbb[...] = dbs[...].astype(BF16)
    me = rep * 4 + dat
    cps = [remote(dbb, dbr.at[d - 1], s_db, v_db, dev) for d, dev in enumerate(others, 1)]
    for c in cps:
        c.start()

    def put_dx(m, v):
        for s in EIGHT:
            for k in FOUR:
                dxo[k, pl.ds(8 * m + s, B, stride=T), :] = v[s * B:(s + 1) * B, k * BLK:(k + 1) * BLK]

    recv_1h(1)
    recv_2x()
    dx_of(0, put_dx)
    recv_1(0, 0)
    send_a1x()
    recv_1(0, 1)
    recv_a1x()
    recv_2(0)
    send_a1(0)
    recv_a2x(1)
    recv_a2x(2)
    remote(dbr, dbr, s_db, v_db, partner).wait_recv()
    tot = dbb[...].astype(F32)
    for d in range(7):
        tot += dbr[d].astype(F32)
    dbo[...] = tot
    recv_a1(0)
    recv_a2(0, 1)
    recv_a2(0, 2)
    for n, sem in ((QTR, s_rp), (W, s_1), (BLK, s_2), (384, s_a), (W, s_rph), (BLK, s_1h), (BLK, s_2x), (384, s_ax)):
        part = dwb.at[0, pl.ds(0, n)]
        remote(part, part, sem, v_p, partner).wait_send()
    remote(hx, hx, s_h, v_p, partner).wait_send()
    remote(zx, zx, s_z, v_p, partner).wait_send()
    for l, snd, rcv in ((0, s_p, v_p), (1, s_px, v_px)):
        half_w = res.at[l, pl.ds(0, H)]
        remote(half_w, half_w, snd, rcv, partner).wait()
    remote(dbr, dbr, s_db, v_db, partner).wait_send()


def out_kernel(res, dbo, dxo, dw_ref, db_ref, dx_ref, buf, dbv, sem, xsem):
    cx = [pltpu.make_async_copy(dxo.at[k], dx_ref.at[:, pl.ds(k * BLK, BLK)], xsem.at[k]) for k in FOUR]
    for l in TWO:
        for j in EIGHT:
            dbv[l:l + 1, W * j:W * j + W] = dbo[8 * l + j:8 * l + j + 1, :]
    cx.append(pltpu.make_async_copy(dbv, db_ref, xsem.at[4]))
    for c in cx:
        c.start()
    n = 64

    def cp(s):
        return pltpu.make_async_copy(buf.at[s], dw_ref.at[s // SUB, rows(lax.rem(s, SUB) * n, n)], sem)

    @loop(32)
    def _(s):
        buf[s] = res[s // SUB, rows(lax.rem(s, SUB) * n, n), :].astype(F32)
        cp(s).start()

    pltpu.make_async_copy(buf, buf, sem).wait()
    for c in cx:
        c.wait()


def solution(mesh):
    vm = pl.BlockSpec(memory_space=pltpu.VMEM)
    hbm = pl.BlockSpec(memory_space=pl.ANY)
    dma, vmem = pltpu.SemaphoreType.DMA, pltpu.VMEM

    def local_step(x, dy, w, b):
        scratch = [
            vmem((2, G), F32),
            vmem((4, R, BLK), BF16), vmem((4, B * PAD, BLK), F32), vmem((4, R, BLK), F32),
            vmem((2, 2, 8, H, W), BF16), vmem((2, 2, G, W), BF16), vmem((3, R + B, H), BF16),
            vmem((2, 4, R, H), F32), vmem((2, R + B, H), F32), vmem((2, R, H), F32),
            vmem((2, 8, R, W), BF16), vmem((R, H), F32), vmem((2, 8, G), F32),
            vmem((SUB, W), F32), vmem((SUB, W), BF16), vmem((7, SUB, W), BF16),
            vmem((2, 2 * H, G), BF16), vmem(P3 + (BLK, HALF), BF16),
            vmem(P3 + (C, HALF), BF16), vmem(P2 + (C, HALF), BF16),
            vmem((3, R, H), BF16), vmem((3, 2, R, W), BF16), vmem((H, QTR), BF16),
            vmem(P2 + (BLK, HALF), BF16), vmem(P2 + (BLK, QTR), BF16), vmem((2, BLK, QTR), BF16),
            vmem((2, BLK, QTR), BF16),
            dma((7,)), dma, dma(P2), dma, dma(P3), dma, dma(P2), dma, dma((2, 3, 2)), dma, dma, dma, dma,
            dma, dma, dma, dma, dma, dma((2,)), dma, dma(P2), dma, dma((4,)), dma, dma((6,)), dma, dma,
        ]
        res, dbo, dxo = pl.pallas_call(
            step_kernel,
            out_shape=(vmem((2, 2 * H, G), BF16), vmem((SUB, W), F32), vmem((4, R, BLK), F32)),
            in_specs=[hbm, hbm, hbm, hbm], out_specs=(vm, vm, vm), scratch_shapes=scratch,
            compiler_params=pltpu.CompilerParams(collective_id=0, has_side_effects=True, vmem_limit_bytes=VMEM_LIMIT),
        )(x.reshape(R, H), dy.reshape(R, H), w, b)
        dw, db, dx = pl.pallas_call(
            out_kernel,
            out_shape=(jax.ShapeDtypeStruct((2, 2 * H, G), F32), jax.ShapeDtypeStruct((2, G), F32),
                       jax.ShapeDtypeStruct((R, H), F32)),
            in_specs=[vm, vm, vm], out_specs=(hbm, hbm, hbm),
            scratch_shapes=[vmem((32, 64, G), F32), vmem((2, G), F32), dma, dma((5,))],
            compiler_params=pltpu.CompilerParams(vmem_limit_bytes=32 * HALF * HALF),
        )(res, dbo, dxo)
        return dw, db, dx.reshape(B, T, H)

    rows_spec = P(("replica", "data"))
    return jax.shard_map(local_step, mesh=mesh, in_specs=(rows_spec, rows_spec, P(), P()),
                         out_specs=(P(), P(), rows_spec), check_vma=False)
```

```python
import jax
import jax.numpy as jnp
from jax import lax
from jax.experimental import pallas as pl
from jax.experimental.pallas import tpu as pltpu
from jax.sharding import PartitionSpec as P

F32, BF16 = jnp.float32, jnp.bfloat16
MESH = pl.DeviceIdType.MESH
T, B, H = 16, 32, 512
G, R = 4 * H, T * B
ORDER = (0, 1, 2, 3)
PAD = 24
MID = 2
CUT = (6, 13)
TWO, THREE, FOUR, EIGHT = range(2), range(3), range(4), range(8)
W = 256
BLK, QTR, HALF, SUB = 128, 512, 1024, 16
P2, P3 = (2, 2), (2, 2, 2)
VMEM_LIMIT = 54 * 1024 * 1024
C = 64


def flip(bit):
    return 1 - bit


def loop(n):
    return pl.loop(0, n)


def dot(a, b):
    return jnp.dot(a, b, preferred_element_type=F32)


def dot_k(a, b, k):
    acc = None
    for i in range(0, a.shape[1], k):
        p = dot(a[:, i:i + k], b[i:i + k])
        acc = p if acc is None else acc + p
    return acc


def dot_nt(a, b):
    return lax.dot_general(a, b, (((1,), (1,)), ((), ())), preferred_element_type=F32)


def sigmoid(z):
    return 0.5 * jnp.tanh(0.5 * z) + 0.5


def rows(start, n, m=SUB):
    return pl.ds(start, n) if isinstance(start, int) else pl.ds(pl.multiple_of(start, m), n)


def step_kernel(x_hbm, dy_hbm, w_hbm, b_hbm, res, dbo, dxo,
                b_ref, xv, xf, dyv, w, wt, hb, gt, cb, tc, dz, eb, dbacc, dbs, dbb, dbr, dwb, rp, r1, r2,
                hx, zx, ub, rph, r1h, r2u, r2h,
                lsem, s_rp, v_rp, s_1, v_1, s_2, v_2, s_a, v_a, s_p, v_p, s_db, v_db,
                s_h, v_h, s_z, v_z, s_rph, v_rph, s_1h, v_1h, s_2x, v_2x, s_ax, v_ax, s_px, v_px):
    rep = lax.axis_index("replica")
    dat = lax.axis_index("data")
    mx, core = dat // 2, dat % 2
    partner = (rep, dat + 1 - 2 * core)
    x_nbr = (rep, lax.rem(dat + 2, 4))
    y_nbr = (flip(rep), dat)
    nbr = ((x_nbr, y_nbr), (y_nbr, x_nbr))
    bits = ((mx, rep), (rep, mx))

    def remote(src, dst, s, v, dev):
        return pltpu.make_async_remote_copy(src_ref=src, dst_ref=dst, send_sem=s, recv_sem=v,
                                            device_id=dev, device_id_type=MESH)

    others = [(lax.rem(rep + (d // 4), 2), lax.rem(dat + (d % 4), 4)) for d in range(1, 8)]
    barrier = pltpu.get_barrier_semaphore()

    ld_x = [pltpu.make_async_copy(x_hbm.at[:, pl.ds(k * BLK, BLK)], xv.at[k], lsem.at[0]) for k in FOUR]
    ld_dy = [pltpu.make_async_copy(dy_hbm.at[:, pl.ds(k * BLK, BLK)], dyv.at[k], lsem.at[1]) for k in FOUR]
    ld_w = [pltpu.make_async_copy(w_hbm.at[l, pl.ds(k * H, H), pl.ds(j * W, W)], w.at[l, k, j],
                                  lsem.at[2 + 2 * l + k])
            for l in TWO for k in TWO for j in EIGHT]
    ld_b = pltpu.make_async_copy(b_hbm, b_ref, lsem.at[6])
    for c in ld_x + [ld_b] + ld_w[:8]:
        c.start()
    for dev in others:
        pl.semaphore_signal(barrier, inc=1, device_id=dev, device_id_type=MESH)
    for l in TWO:
        hb[l + 1, pl.ds(0, B), :] = jnp.zeros((B, H), BF16)
        cb[l, pl.ds(0, B), :] = jnp.zeros((B, H), F32)
    pltpu.make_async_copy(xv, xv, lsem.at[0]).wait()
    for c in ld_w[8:SUB]:
        c.start()
    for i in range(B):
        xf[:, i * PAD:i * PAD + T, :] = xv[:, i * T:(i + 1) * T, :].astype(F32)

    @loop(T)
    def _(t):
        hb[0, rows((t + 1) * B, B), :] = jnp.concatenate(
            [xf[k, pl.ds(t, B, stride=PAD), :] for k in FOUR], axis=1).astype(BF16)
    for c in ld_w[SUB:] + ld_dy:
        c.start()

    def wait_w(l, k):
        pltpu.make_async_copy(w.at[l, k], w.at[l, k], lsem.at[2 + 2 * l + k]).wait()

    ld_b.wait()
    pltpu.make_async_copy(w.at[0, 0], w.at[0, 0], lsem.at[2]).wait()

    def in_block(l, s, n, m=BLK):
        r0 = rows(s * BLK, m)
        gt[l, n // 2, r0, W * (n % 2):W * (n % 2) + W] = (
            dot(hb[l, rows(B + s * BLK, m), :], w[l, 0, n]) + b_ref[l:l + 1, W * n:W * n + W])

    def transpose_rec(l, j, n):
        wt[l, n, rows(j * W, W), :] = w[l, 1, j, pl.ds(n * W, W), :].T

    def step_dots(l, t, h):
        zin = [gt[l, k, rows(t * B, B), :] for k in FOUR]
        prod = [None] * 8
        if h is None:
            return zin, prod
        for k in (0, 2, 1, 3):
            for n in TWO:
                prod[2 * k + n] = dot_k(h, w[l, 1, 2 * k + n], BLK)
        return zin, prod

    def step_gates(l, t, zp, c):
        zin, prod = zp
        r0, r1_ = rows(t * B, B), rows((t + 1) * B, B)
        hs, cs = [], []
        for n in TWO:
            m = slice(W * n, W * n + W)
            z = [zin[k][:, m] if prod[2 * k + n] is None else zin[k][:, m] + prod[2 * k + n] for k in FOUR]
            i, g, f, o = sigmoid(z[0]), jnp.tanh(z[2]), sigmoid(z[1]), sigmoid(z[3])
            cn = f * c[:, m] + i * g
            th = jnp.tanh(cn)
            hn = (o * th).astype(BF16)
            for k, v in enumerate((i, f, g, o)):
                gt[l, k, r0, m] = v
            cb[l, r1_, m] = cn
            tc[l, r0, m] = th
            hb[l + 1, r1_, m] = hn
            hs.append(hn)
            cs.append(cn)
        return jnp.concatenate(hs, axis=1), jnp.concatenate(cs, axis=1)

    zero_state = (jnp.zeros((B, H), BF16), jnp.zeros((B, H), F32))
    def pick(a, b):
        return a + core * (b - a)

    u_b1, u_b2 = pick(mx, rep), pick(rep, mx)
    u_n1 = (pick(rep, flip(rep)), pick(lax.rem(dat + 2, 4), dat))
    u_n2 = (pick(flip(rep), rep), pick(dat, lax.rem(dat + 2, 4)))
    x_core0, y_core1 = (rep, 2 * (flip(mx))), (flip(rep), 2 * mx + 1)
    dests = ((partner, 0, pick(4 + 2 * rep, 2 * mx)), (x_core0, 1 + core, 2 * (flip(mx))), (y_core1, 1 + core, 4 + 2 * (flip(rep))))
    u_col = pick(2 * mx, 4 + 2 * rep)

    def send_h(r0, n):
        for dev, slot, _ in dests:
            remote(hb.at[1, rows(B + r0, n)], hx.at[slot, rows(r0, n)], s_h, v_h, dev).start()

    def send_z(r0, n):
        for dev, slot, c0 in dests:
            remote(dz.at[1, pl.ds(c0, 2), rows(r0, n)], zx.at[slot, :, rows(r0, n)], s_z, v_z, dev).start()

    for n in EIGHT:
        in_block(0, 0, n)
    h0, c0 = None, zero_state[1]
    for q in FOUR:
        if q == 1:
            wait_w(0, 1)
        zp = step_dots(0, q, h0)
        if q == 0:
            for n in EIGHT:
                in_block(0, 2, n, 2 * BLK)
        in_block(0, 1, 2 * q)
        in_block(0, 1, 2 * q + 1)
        if q:
            transpose_rec(0, q // 2, q % 2)
        if q == 1:
            transpose_rec(0, 0, 0)
        h0, c0 = step_gates(0, q, zp, c0)
        if q == 1:
            pl.semaphore_wait(barrier, 7)
            send_h(0, 2 * B)
    wait_w(1, 0)
    wait_w(1, 1)

    def both(s, carry, first=False, last=False):
        h0, c0, h1, c1 = carry
        t0, t1 = 4 * s + 4, 4 * s
        if first:
            send_h(2 * B, 2 * B)
        a = step_dots(0, t0, h0)
        for n in EIGHT:
            in_block(1, s, n)
        h0, c0 = step_gates(0, t0, a, c0)
        for q in FOUR:
            if q < 3:
                a = step_dots(0, t0 + q + 1, h0)
            b = step_dots(1, t1 + q, h1)
            if q < 3:
                h0, c0 = step_gates(0, t0 + q + 1, a, c0)
            transpose_rec(0, 2 * s + 2 + q // 2, q % 2)
            transpose_rec(1, 2 * s + q // 2, q % 2)
            h1, c1 = step_gates(1, t1 + q, b, c1)
            if q == MID:
                send_h(t0 * B, BLK)
        return h0, c0, h1, c1

    carry = both(0, (h0, c0, None, zero_state[1]), first=True)
    carry = both(1, carry)
    h0, c0, h1, c1 = both(2, carry, last=True)
    for q in FOUR:
        zp = step_dots(1, 12 + q, h1)
        if q == 0:
            for n in EIGHT:
                in_block(1, 3, n)
            zp = [gt[1, k, rows(12 * B, B), :] for k in FOUR], zp[1]
        transpose_rec(1, 6 + q // 2, q % 2)
        h1, c1 = step_gates(1, 12 + q, zp, c1)

    pltpu.make_async_copy(dyv, dyv, lsem.at[1]).wait()
    dbacc[...] = jnp.zeros_like(dbacc)

    def bwd_layer(l, e_of, halfway=None, after=None):
        def body(s, carry):
            r, dc_next = carry
            t = T - 1 - s
            r0 = rows(t * B, B)
            i, f, g, o = [gt[l, k, r0, :] for k in FOUR]
            th, c_prev = tc[l, r0, :], cb[l, r0, :]
            dh = e_of(t) + r
            dc = dc_next + dh * o * (1.0 - th * th)
            dzs = (dc * g * i * (1.0 - i), dc * c_prev * f * (1.0 - f), dc * i * (1.0 - g * g), dh * th * o * (1.0 - o))
            acc = None
            for k in ORDER:
                d = dzs[k]
                dbacc[l, :, k * H:(k + 1) * H] += d[0:8] + d[8:SUB] + d[SUB:24] + d[24:32]
                d16 = d.astype(BF16)
                for n in TWO:
                    dz[l, 2 * k + n, r0, :] = d16[:, W * n:W * n + W]
                p = [dot_k(d16, wt[l, n, pl.ds(k * H, H), :], BLK) for n in TWO]
                acc = p if acc is None else [a + b for a, b in zip(acc, p)]
            return jnp.concatenate(acc, axis=1), dc * f

        zero = jnp.zeros((B, H), F32)
        carry = (zero, zero)
        if after is not None:
            def step_and_send(s, carry):
                carry = body(s, carry)
                after((T - 1 - s) * B)
                return carry
            lax.fori_loop(0, T, step_and_send, carry)
        else:
            carry = lax.fori_loop(0, CUT[0], body, carry)
            halfway(0)
            carry = lax.fori_loop(CUT[0], CUT[1], body, carry)
            halfway(1)
            lax.fori_loop(CUT[1], T, body, carry)

    def dx_of(l, put):
        acc = None
        for m in TWO:
            rr = pl.ds(m * W, W)
            acc = None
            for j in EIGHT:
                p = dot_nt(dz[l, j, rr, :], w[l, 0, j])
                acc = p if acc is None else acc + p
            put(m, acc)

    def block_row(who, q, grp):
        b1 = bits[q][0]
        part = flip(b1) if grp == 0 else b1
        return who * H + q * W + part * BLK

    def cols(half):
        return pl.ds(pl.multiple_of(half * HALF, HALF), HALF)

    def half_of(q, h):
        b2 = bits[q][1]
        return flip(b2) if h == 0 else b2

    def lhs_of(l, who, q, grp):
        r0 = block_row(who, q, grp)
        return hb[l + who, rows(B * (flip(who)), R, B), rows(r0 - who * H, BLK, BLK)].T

    def dw_block(l, who, q, grp, h):
        lt = lhs_of(l, who, q, grp)
        half = half_of(q, h)
        for n in FOUR:
            dwb[l, rows(block_row(who, q, grp), BLK), pl.ds(pl.multiple_of(half * HALF + n * W, W), W)] = (
                dot(lt, dz[l, 4 * half + n]).astype(BF16))

    def cp_rp(l, q, grp, h):
        rr, cc = rows(block_row(flip(core), q, grp), BLK), cols(half_of(q, h))
        return remote(dwb.at[l, rr, cc], rp.at[q, grp, h], s_rp, v_rp.at[grp, h], partner)

    def add_rp(l, q, grp, h):
        r0, cc = block_row(core, q, grp), cols(half_of(q, h))

        @loop(4)
        def _(i):
            rr = rows(r0 + i * 32, 32)
            dwb[l, rr, cc] = (dwb[l, rr, cc].astype(F32) + rp[q, grp, h, rows(i * 32, 32), :].astype(F32)).astype(BF16)

    def place(q, grp, h, i):
        return rows(block_row(core, q, grp) + C * i, C), cols(half_of(q, h))

    def cp_1(l, q, h, i):
        rr, cc = place(q, 0, h, i)
        return remote(dwb.at[l, rr, cc], r1.at[q, h, i], s_1, v_1.at[q, h, i], nbr[q][0])

    def cp_2(l, q, i):
        rr, cc = place(q, 1, 0, i)
        return remote(dwb.at[l, rr, cc], r2.at[q, i], s_2, v_2.at[q, i], nbr[q][1])

    def fin(q, k, i):
        b1, b2 = bits[q]
        c1 = b1 if k in (0, 1) else flip(b1)
        c2 = b2 if k in (0, 2) else flip(b2)
        return rows(core * H + q * W + c1 * BLK + C * i, C), cols(c2)

    def cp_a(l, q, k, i):
        rr, cc = fin(q, 1 if k == 2 else 0, i)
        return remote(res.at[l, rr, cc], res.at[l, rr, cc], s_a, v_a.at[q, k, i], nbr[q][1 if k == 0 else 0])

    def cp_p(l, q, k, i):
        rr, cc = fin(q, k, i)
        return remote(res.at[l, rr, cc], res.at[l, rr, cc], s_p, v_p, partner)

    QI = [(q, i) for i in TWO for q in TWO]

    def dw_pair(l, who, grp, h):
        for q in TWO:
            dw_block(l, who, q, grp, h)
            if who is not core:
                cp_rp(l, q, grp, h).start()

    def take_rp(l, grp, h):
        pair = rp.at[:, grp, h]
        remote(pair, pair, s_rp, v_rp.at[grp, h], partner).wait_recv()
        for q in TWO:
            add_rp(l, q, grp, h)
            if grp == 0:
                for i in TWO:
                    cp_1(l, q, h, i).start()

    def grads_send(l):
        other = flip(core)
        dw_pair(l, other, 0, 0)
        dw_pair(l, core, 0, 0)
        dw_pair(l, other, 0, 1)
        take_rp(l, 0, 0)
        dw_pair(l, core, 0, 1)
        dw_pair(l, other, 1, 0)
        take_rp(l, 0, 1)
        dw_pair(l, core, 1, 0)
        dw_pair(l, other, 1, 1)
        dw_pair(l, core, 1, 1)

    def recv_1(l, h):
        if h == 0:
            take_rp(l, 1, 0)
            take_rp(l, 1, 1)
        for q, i in QI:
            cp_1(l, q, h, i).wait_recv()
            rr, cc = place(q, 1, h, i)
            dwb[l, rr, cc] = (dwb[l, rr, cc].astype(F32) + r1[q, h, i].astype(F32)).astype(BF16)
            if h == 0:
                cp_2(l, q, i).start()

    def recv_2(l):
        for q, i in QI:
            cp_2(l, q, i).wait_recv()
            rr, cc = fin(q, 0, i)
            res[l, rr, cc] = (dwb[l, rr, cc].astype(F32) + r2[q, i].astype(F32)).astype(BF16)
            cp_a(l, q, 0, i).start()
            cp_p(l, q, 0, i).start()

    def send_a1(l):
        for q, i in QI:
            cp_a(l, q, 1, i).start()

    def recv_a1(l):
        for q, i in QI:
            cp_a(l, q, 0, i).wait_recv()
            cp_a(l, q, 2, i).start()
            cp_p(l, q, 1, i).start()

    def recv_a2(l, k):
        for q, i in QI:
            cp_a(l, q, k, i).wait_recv()
            cp_p(l, q, k + 1, i).start()

    def h_row(who, q):
        return H + who * W + q * BLK

    def dwh_block(who, q, grp):
        lt = hb[2, pl.ds(0, R), rows(h_row(who, q) - H, BLK, BLK)].T
        half = flip(bits[q][0]) if grp == 0 else bits[q][0]
        for n in FOUR:
            dwb[1, rows(h_row(who, q), BLK), pl.ds(pl.multiple_of(half * HALF + n * W, W), W)] = (
                dot(lt, dz[1, 4 * half + n]).astype(BF16))

    def cp_rph(q, grp):
        half = flip(bits[q][0]) if grp == 0 else bits[q][0]
        return remote(dwb.at[1, rows(h_row(flip(core), q), BLK), cols(half)], rph.at[q, grp], s_rph, v_rph.at[grp], partner)

    def quarter(q, grp, h):
        half = flip(bits[q][0]) if grp == 0 else bits[q][0]
        return pl.ds(pl.multiple_of(half * HALF + QTR * half_of(q, h), QTR), QTR)

    def cp_1h(q, h):
        return remote(dwb.at[1, rows(h_row(core, q), BLK), quarter(q, 0, h)], r1h.at[q, h], s_1h, v_1h.at[q, h], nbr[q][0])

    def take_rph(grp):
        pair = rph.at[:, grp]
        remote(pair, pair, s_rph, v_rph.at[grp], partner).wait_recv()
        for q in TWO:
            r0, cc = h_row(core, q), cols(flip(bits[q][0]) if grp == 0 else bits[q][0])

            @loop(4)
            def _(i):
                rr = rows(r0 + i * 32, 32)
                dwb[1, rr, cc] = (dwb[1, rr, cc].astype(F32) + rph[q, grp, rows(i * 32, 32), :].astype(F32)).astype(BF16)
            if grp == 0:
                for h in TWO:
                    cp_1h(q, h).start()

    def grads_send_1():
        for grp in TWO:
            for q in TWO:
                dwh_block(flip(core), q, grp)
                cp_rph(q, grp).start()
            for q in TWO:
                dwh_block(core, q, grp)
            if grp == 0:
                take_rph(0)

    def sum_u():
        remote(hx, hx, s_h, v_h, partner).wait_recv()
        remote(zx, zx, s_z, v_z, partner).wait_recv()
        for m in FOUR:
            f0 = pl.ds(m * BLK, BLK)
            lts = [hb[1, pl.ds(B, R), f0].T] + [hx[i, :, f0].T for i in THREE]
            for n in TWO:
                zs = [dz[1, u_col + n]] + [zx[i, n] for i in THREE]
                acc = None
                for lt, z in zip(lts, zs):
                    p = dot(lt, z).astype(BF16).astype(F32)
                    acc = p if acc is None else acc + p
                ub[f0, W * n:W * n + W] = acc.astype(BF16)

    def item_nbr(j):
        return (u_n1, u_n2) if j < 2 else nbr[j - 2]

    def item_fin(j, k):
        b1, b2 = (u_b1, u_b2) if j < 2 else bits[j - 2]
        c1 = b1 if k in (0, 1) else flip(b1)
        c2 = b2 if k in (0, 2) else flip(b2)
        if j < 2:
            return rows(W * c2 + BLK * j, BLK), pl.ds(pl.multiple_of(core * HALF + QTR * c1, QTR), QTR)
        return rows(h_row(core, j - 2), BLK), pl.ds(pl.multiple_of(HALF * c1 + QTR * c2, QTR), QTR)

    def cp_2x(j):
        if j < 2:
            src, dst = ub.at[rows(W * (flip(u_b2)) + BLK * j, BLK)], r2u.at[j]
        else:
            src, dst = dwb.at[1, rows(h_row(core, j - 2), BLK), quarter(j - 2, 1, 0)], r2h.at[j - 2]
        return remote(src, dst, s_2x, v_2x.at[j], item_nbr(j)[1])

    def cp_ax(j, k):
        rr, cc = item_fin(j, 1 if k == 2 else 0)
        return remote(res.at[1, rr, cc], res.at[1, rr, cc], s_ax, v_ax.at[j if k == 0 else 3 + k], item_nbr(j)[1 if k == 0 else 0])

    def cp_px(j, k):
        rr, cc = item_fin(j, k)
        return remote(res.at[1, rr, cc], res.at[1, rr, cc], s_px, v_px, partner)

    JS = (2, 3, 0, 1)

    def recv_1h(h):
        if h == 0:
            take_rph(1)
        for q in TWO:
            cp_1h(q, h).wait_recv()
            rr, cc = rows(h_row(core, q), BLK), quarter(q, 1, h)
            dwb[1, rr, cc] = (dwb[1, rr, cc].astype(F32) + r1h[q, h].astype(F32)).astype(BF16)
            if h == 0:
                cp_2x(2 + q).start()

    def recv_2x():
        for j in JS:
            cp_2x(j).wait_recv()
            rr, cc = item_fin(j, 0)
            if j < 2:
                mine, got = ub[rows(W * u_b2 + BLK * j, BLK), :], r2u[j]
            else:
                mine, got = dwb[1, rr, cc], r2h[j - 2]
            res[1, rr, cc] = (mine.astype(F32) + got.astype(F32)).astype(BF16)
            cp_ax(j, 0).start()
            cp_px(j, 0).start()

    def send_a1x():
        for j in JS:
            cp_ax(j, 1).start()

    def recv_a1x():
        for j in JS:
            cp_ax(j, 0).wait_recv()
            cp_ax(j, 2).start()
            cp_px(j, 1).start()

    def recv_a2x(k):
        part = res.at[1, pl.ds(0, BLK)]
        remote(part, part, s_ax, v_ax.at[3 + k], partner).wait_recv()
        for j in JS:
            cp_px(j, k + 1).start()

    def between(part):
        if part == 0:
            sum_u()
            for j in TWO:
                cp_2x(j).start()
        else:
            recv_1h(0)

    bwd_layer(1, lambda t: jnp.concatenate([dyv[k, pl.ds(t, B, stride=T), :] for k in FOUR], axis=1), after=lambda r0: send_z(r0, B))
    grads_send_1()

    def put_e(m, v):
        eb[pl.ds(m * W, W), :] = v
    dx_of(1, put_e)
    bwd_layer(0, lambda t: eb[rows(t * B, B), :], between)
    grads_send(0)

    for l in TWO:
        for j in EIGHT:
            dbs[8 * l + j:8 * l + j + 1, :] = jnp.sum(dbacc[l, :, W * j:W * j + W], axis=0, keepdims=True)
    dbb[...] = dbs[...].astype(BF16)
    me = rep * 4 + dat
    cps = [remote(dbb, dbr.at[d - 1], s_db, v_db, dev) for d, dev in enumerate(others, 1)]
    for c in cps:
        c.start()

    def put_dx(m, v):
        for s in EIGHT:
            for k in FOUR:
                dxo[k, pl.ds(8 * m + s, B, stride=T), :] = v[s * B:(s + 1) * B, k * BLK:(k + 1) * BLK]

    recv_1h(1)
    recv_2x()
    dx_of(0, put_dx)
    recv_1(0, 0)
    send_a1x()
    recv_1(0, 1)
    recv_a1x()
    recv_2(0)
    send_a1(0)
    recv_a2x(1)
    recv_a2x(2)
    remote(dbr, dbr, s_db, v_db, partner).wait_recv()
    tot = dbb[...].astype(F32)
    for d in range(7):
        tot += dbr[d].astype(F32)
    dbo[...] = tot
    recv_a1(0)
    recv_a2(0, 1)
    recv_a2(0, 2)
    for n, sem in ((QTR, s_rp), (W, s_1), (BLK, s_2), (384, s_a), (W, s_rph), (BLK, s_1h), (BLK, s_2x), (384, s_ax)):
        part = dwb.at[0, pl.ds(0, n)]
        remote(part, part, sem, v_p, partner).wait_send()
    remote(hx, hx, s_h, v_p, partner).wait_send()
    remote(zx, zx, s_z, v_p, partner).wait_send()
    for l, snd, rcv in ((0, s_p, v_p), (1, s_px, v_px)):
        half_w = res.at[l, pl.ds(0, H)]
        remote(half_w, half_w, snd, rcv, partner).wait()
    remote(dbr, dbr, s_db, v_db, partner).wait_send()


def out_kernel(res, dbo, dxo, dw_ref, db_ref, dx_ref, buf, dbv, sem, xsem):
    cx = [pltpu.make_async_copy(dxo.at[k], dx_ref.at[:, pl.ds(k * BLK, BLK)], xsem.at[k]) for k in FOUR]
    for l in TWO:
        for j in EIGHT:
            dbv[l:l + 1, W * j:W * j + W] = dbo[8 * l + j:8 * l + j + 1, :]
    cx.append(pltpu.make_async_copy(dbv, db_ref, xsem.at[4]))
    for c in cx:
        c.start()
    n = 64

    def cp(s):
        return pltpu.make_async_copy(buf.at[s], dw_ref.at[s // SUB, rows(lax.rem(s, SUB) * n, n)], sem)

    @loop(32)
    def _(s):
        buf[s] = res[s // SUB, rows(lax.rem(s, SUB) * n, n), :].astype(F32)
        cp(s).start()

    pltpu.make_async_copy(buf, buf, sem).wait()
    for c in cx:
        c.wait()


def solution(mesh):
    vm = pl.BlockSpec(memory_space=pltpu.VMEM)
    hbm = pl.BlockSpec(memory_space=pl.ANY)
    dma, vmem = pltpu.SemaphoreType.DMA, pltpu.VMEM

    def local_step(x, dy, w, b):
        scratch = [
            vmem((2, G), F32),
            vmem((4, R, BLK), BF16), vmem((4, B * PAD, BLK), F32), vmem((4, R, BLK), F32),
            vmem((2, 2, 8, H, W), BF16), vmem((2, 2, G, W), BF16), vmem((3, R + B, H), BF16),
            vmem((2, 4, R, H), F32), vmem((2, R + B, H), F32), vmem((2, R, H), F32),
            vmem((2, 8, R, W), BF16), vmem((R, H), F32), vmem((2, 8, G), F32),
            vmem((SUB, W), F32), vmem((SUB, W), BF16), vmem((7, SUB, W), BF16),
            vmem((2, 2 * H, G), BF16), vmem(P3 + (BLK, HALF), BF16),
            vmem(P3 + (C, HALF), BF16), vmem(P2 + (C, HALF), BF16),
            vmem((3, R, H), BF16), vmem((3, 2, R, W), BF16), vmem((H, QTR), BF16),
            vmem(P2 + (BLK, HALF), BF16), vmem(P2 + (BLK, QTR), BF16), vmem((2, BLK, QTR), BF16),
            vmem((2, BLK, QTR), BF16),
            dma((7,)), dma, dma(P2), dma, dma(P3), dma, dma(P2), dma, dma((2, 3, 2)), dma, dma, dma, dma,
            dma, dma, dma, dma, dma, dma((2,)), dma, dma(P2), dma, dma((4,)), dma, dma((6,)), dma, dma,
        ]
        res, dbo, dxo = pl.pallas_call(
            step_kernel,
            out_shape=(vmem((2, 2 * H, G), BF16), vmem((SUB, W), F32), vmem((4, R, BLK), F32)),
            in_specs=[hbm, hbm, hbm, hbm], out_specs=(vm, vm, vm), scratch_shapes=scratch,
            compiler_params=pltpu.CompilerParams(collective_id=0, has_side_effects=True, vmem_limit_bytes=VMEM_LIMIT),
        )(x.reshape(R, H), dy.reshape(R, H), w, b)
        dw, db, dx = pl.pallas_call(
            out_kernel,
            out_shape=(jax.ShapeDtypeStruct((2, 2 * H, G), F32), jax.ShapeDtypeStruct((2, G), F32),
                       jax.ShapeDtypeStruct((R, H), F32)),
            in_specs=[vm, vm, vm], out_specs=(hbm, hbm, hbm),
            scratch_shapes=[vmem((32, 64, G), F32), vmem((2, G), F32), dma, dma((5,))],
            compiler_params=pltpu.CompilerParams(vmem_limit_bytes=32 * HALF * HALF),
        )(res, dbo, dxo)
        return dw, db, dx.reshape(B, T, H)

    rows_spec = P(("replica", "data"))
    return jax.shard_map(local_step, mesh=mesh, in_specs=(rows_spec, rows_spec, P(), P()),
                         out_specs=(P(), P(), rows_spec), check_vma=False)
```
